32 devices in a mesh: section: 2 (over y), freq: 16 (over z, x, core).
Axes of the slice: x: 2, y: 2, z: 4, core: 2. Of those that a mesh axis runs over, the one named last changes fastest.
Arguments:
- spectra: float32 [4, 16, 131072], P('section', None, 'freq'), may hold values from 0.1 to 90, as said below
- channel_gain: float32 [131072], P('freq'), may hold values from 0.5 to 2
- bandpass_bin: int32 [131072], P('freq'), may hold values from 0 to 63, never falling along the last dimension, each value on 1 to 8192 neighbouring positions
- drift_range: int32 [4], replicated, may hold values from 1 to 2, as said below
- hit_cutoff: int32 [4, 2, 16], replicated, may hold values from 0 to 1023
Outputs:
- drift_score: float32 [4, 2, 131072], P(None, 'section', 'freq')
The draws below stay inside these ranges and needn't reach their ends.
Inputs may be any that keep to these rules, and one draw needn't show every extreme that they name: `spectra`: every entry is positive. `bandpass_bin`: the bins never fall along the channels and each of the 64 bins holds 1 to 8192 channels. `drift_range`: some group reaches 2 and some other group searches stride 1 only.
All inputs are finite; a program needn't handle non-finite values.
Results may differ from the reference program's by a relative error of at most 0.0003.
Values sent between devices are 32-bit elements; how exact they have to be, the bound alone decides.
No kernel may reach another device: no remote copies, remote signals or barrier semaphores. Data moves between devices by JAX's collectives and lax.ppermute only.
A program may use at most 64 MiB of HBM per device.

```python
import math
import jax
import jax.numpy as jnp
import numpy as np
from jax import lax

INTEG = 16
F_DEV = 8192
KMAX = 2
CHANNELS = 131072
GROUPS = 4
BINS = 64


def draw_spectra(key, part):
    first_key, second_key = jax.random.split(jax.random.fold_in(key, 11))
    group_ramp = 1.0 + 2.0 * jnp.arange(GROUPS, dtype=jnp.float32) / max(GROUPS - 1, 1)
    chan_ramp = 1.0 + 2.0 * jnp.arange(CHANNELS, dtype=jnp.float32) / (CHANNELS - 1)
    channel_scale = jnp.exp(jax.random.uniform(first_key, (GROUPS, 1, CHANNELS), jnp.float32, -1.2, 1.2))
    element = jax.random.uniform(second_key, (GROUPS, INTEG, CHANNELS), jnp.float32, 0.5, 1.5)
    result_array = channel_scale * element * group_ramp[:, None, None] * chan_ramp[None, None, :]
    return result_array.astype(jnp.float32)


def draw_drift_range(key, part):
    reach_all = jax.random.randint(jax.random.fold_in(key, 21), (GROUPS,), 1, KMAX + 1).astype(jnp.int32)
    chosen = jax.random.randint(jax.random.fold_in(key, 22), (), 0, GROUPS).astype(jnp.int32)
    step_over = jax.random.randint(jax.random.fold_in(key, 23), (), 1, GROUPS).astype(jnp.int32)
    lowest = (chosen + step_over) % GROUPS
    reach_all = reach_all.at[chosen].set(KMAX)
    reach_all = reach_all.at[lowest].set(1)
    return reach_all.astype(jnp.int32)


def place_ends(array, key, smallest, top_value):
    longest = array.shape.index(max(array.shape))
    spots = []
    for shift in (0, 1):
        where = [jax.random.randint(jax.random.fold_in(key, axis), (), 0, length) for axis, length in enumerate(array.shape)]
        where[longest] = (where[longest] + shift) % array.shape[longest]
        spots.append(tuple(where))
    return array.at[spots[0]].set(smallest).at[spots[1]].set(top_value)


def block_levels(rng, extent, pieces, low, top_value):
    level = 1.0
    for dim, shards_of in pieces:
        draws = jax.random.uniform(jax.random.fold_in(jax.random.fold_in(rng, 6), dim), (shards_of,), jnp.float32, low / len(pieces), top_value / len(pieces))
        level = level * jnp.repeat(jnp.exp(draws), extent[dim] // shards_of).reshape((-1,) + (1,) * (len(extent) - 1 - dim))
    return level


def split_up(amount, total, reach, lean):
    weights = [(1 << 20) // math.isqrt(grade ** lean) + 1 for grade in range(2, amount + 1)]
    rest, counts = total - reach - (amount - 1), [1] * (amount - 1)
    while rest > 0:
        movable = [i for i in range(amount - 1) if counts[i] < reach]
        pool, left = sum([weights[i] for i in movable]), rest
        for i in movable:
            addition = min(reach - counts[i], max(1, left * weights[i] // pool), rest)
            counts[i] = counts[i] + addition
            rest = rest - addition
    return np.array([reach] + counts)


def uneven_parts(own_key, amount, total, reach, lean):
    if amount == 2:
        one = jax.random.randint(own_key, (), max(1, total - reach), min(reach, total - 1) + 1)
        return jnp.stack([one, total - one])
    lengths = jnp.asarray(split_up(amount, total, reach, lean), jnp.int32)
    twos = (amount - 1) // 2
    giver, sink = lengths[1:1 + 2 * twos:2], lengths[2:2 + 2 * twos:2]
    slack = jnp.minimum(giver - 1, reach - sink)
    shifted = jax.random.randint(jax.random.fold_in(own_key, 1), (twos,), 0, 1 << 20) % (slack + 1)
    lengths = lengths.at[1:1 + 2 * twos:2].set(giver - shifted).at[2:2 + 2 * twos:2].set(sink + shifted)
    return lengths[jax.random.permutation(jax.random.fold_in(own_key, 2), amount)]


def setup_inputs(seed: int = 0) -> dict:
    key_of = jax.random.split(jax.random.key(seed), 6)
    return {
        "spectra": draw_spectra(jax.random.fold_in(key_of[5], 71), 0),
        "channel_gain": jnp.clip(jnp.exp(math.log(2.0) - 1.3862944 * jax.random.uniform(key_of[1], (CHANNELS,), jnp.float32) ** block_levels(key_of[1], (CHANNELS,), ((0, 16),), -0.2, 0.2)), 0.5, 2.0),
        "bandpass_bin": jnp.searchsorted(jnp.cumsum(uneven_parts(key_of[2], BINS, CHANNELS, F_DEV, 0)), jnp.arange(CHANNELS), side="right").astype(jnp.int32),
        "drift_range": draw_drift_range(jax.random.fold_in(key_of[5], 71), 0),
        "hit_cutoff": place_ends(jax.random.randint(key_of[4], (GROUPS, KMAX, INTEG), 0, 1024), jax.random.fold_in(key_of[4], 1), 0, 1023).astype(jnp.int32),
    }


def taylor_tree(extended, stride, margin):
    length = extended.shape[-1]
    current = extended[:, None, :]
    blocks_width = 1
    while current.shape[0] > 1:
        former = current[0::2]
        latter = jnp.pad(current[1::2], ((0, 0), (0, 0), (0, margin)))
        merged = []
        for half_idx in range(blocks_width):
            anchor = former[:, half_idx]
            source = latter[:, half_idx]
            merged.append(anchor + lax.dynamic_slice_in_dim(source, half_idx * stride, length, axis=1))
            merged.append(anchor + lax.dynamic_slice_in_dim(source, (half_idx + 1) * stride, length, axis=1))
        current = jnp.stack(merged, axis=1)
        blocks_width = blocks_width * 2
    return current[0]


def score_rate(extended, stride, cut_row, chan_dev, margin):
    drifts = taylor_tree(extended, stride, margin)[:, :chan_dev]
    cut_levels = cut_row.astype(jnp.float32) / 256.0
    return jnp.mean(jax.nn.relu(0.25 * drifts - cut_levels[:, None]), axis=0)


def reference(spectra, channel_gain, bandpass_bin, drift_range, hit_cutoff):
    calibrated = spectra * channel_gain[None, None, :]
    summed = jnp.sum(calibrated, axis=1)
    bin_sums = jax.ops.segment_sum(summed.T, bandpass_bin, num_segments=BINS, indices_are_sorted=True).T
    tally_row = jax.ops.segment_sum(jnp.full(bandpass_bin.shape, float(INTEG), jnp.float32), bandpass_bin, num_segments=BINS, indices_are_sorted=True)
    tallies = jnp.broadcast_to(tally_row[None, :], bin_sums.shape)
    running = jnp.cumsum(bin_sums, axis=0) / jnp.cumsum(tallies, axis=0)
    levels = jnp.take(running, bandpass_bin, axis=1)
    normal = calibrated / levels[:, None, :] - 1.0
    margin = KMAX * (INTEG - 1)

    def per_group(group_items):
        data_rows, reach_max, cut_rows = group_items
        extended = jnp.pad(data_rows, ((0, 0), (0, margin)))
        rate_rows = []
        for stride in range(1, KMAX + 1):
            rate_rows.append(lax.cond(stride <= reach_max,
                                      lambda: score_rate(extended, stride, cut_rows[stride - 1], CHANNELS, margin),
                                      lambda: jnp.zeros((CHANNELS,), jnp.float32)))
        return jnp.stack(rate_rows)

    return lax.map(per_group, (normal, drift_range, hit_cutoff))
```

```python
import functools

import jax
import jax.numpy as jnp
from jax import lax
from jax.experimental import pallas as pl
from jax.experimental.pallas import tpu as pltpu
from jax.sharding import PartitionSpec as P

LANES = 128
SUBS = 8
BOTH = ("section", "freq")
CHUNK = 8
VMEM = pl.BlockSpec(memory_space=pltpu.VMEM)
SMEM = pl.BlockSpec(memory_space=pltpu.SMEM)
PARAMS = pltpu.CompilerParams(vmem_limit_bytes=16 * 2**20)


def lane_iota():
    return lax.broadcasted_iota(jnp.int32, (SUBS, LANES), 1)


def row_iota():
    return lax.broadcasted_iota(jnp.int32, (SUBS, LANES), 0)


def row_tile(ref, base, tile, tiles):
    return ref[pl.ds(base + tile, SUBS, stride=tiles), :]


def spectra_tile(x_ref, group, t, tile, cols, integrations):
    tiles = cols // SUBS
    block = group * (integrations // SUBS) + t // SUBS
    start = (block * cols + tile) * SUBS + t % SUBS
    return x_ref[pl.ds(start, SUBS, stride=tiles * SUBS), :]


def bin_kernel(groups, integrations, bin_tiles, x_ref, gain_ref, bins_ref, table_ref, rim_ref):
    cols = gain_ref.shape[0]
    tiles = cols // SUBS
    lane, row = lane_iota(), row_iota()
    for group in range(groups):
        for block in range(integrations // SUBS):
            at = group * (integrations // SUBS) + block
            rim_ref[at * SUBS : (at + 1) * SUBS, :] = (
                x_ref[at * cols * SUBS : at * cols * SUBS + SUBS, :] * gain_ref[0:1, :]
            )
    last_rows = groups * integrations
    rim_ref[last_rows : last_rows + SUBS, :] = jnp.broadcast_to(
        bins_ref[0:1, :].astype(jnp.float32), (SUBS, LANES)
    )
    bins = [row_tile(bins_ref, 0, tile, tiles) for tile in range(tiles)]
    summed = []
    for group in range(groups):
        for tile in range(tiles):
            total = spectra_tile(x_ref, group, 0, tile, cols, integrations)
            for t in range(1, integrations):
                total = total + spectra_tile(x_ref, group, t, tile, cols, integrations)
            summed.append(total * row_tile(gain_ref, 0, tile, tiles))
    first, last = jnp.min(bins[0]), jnp.max(bins[-1])

    def some_bins(step, tables):
        for u in range(CHUNK):
            b = first + step * CHUNK + u
            masks = [part == b for part in bins]
            stacked = jnp.zeros((SUBS, LANES), jnp.float32)
            for quantity in range(groups + 1):
                partial = jnp.zeros((SUBS, LANES), jnp.float32)
                for tile in range(tiles):
                    value = 1.0 if quantity == groups else summed[quantity * tiles + tile]
                    partial = partial + jnp.where(masks[tile], value, 0.0)
                stacked = jnp.where(row == quantity, jnp.sum(partial, axis=0, keepdims=True), stacked)
            total = jnp.sum(stacked, axis=1, keepdims=True)
            tables = tuple(
                table + jnp.where(lane == b - q * LANES, total, 0.0) for q, table in enumerate(tables)
            )
        return tables

    start = tuple(jnp.zeros((SUBS, LANES), jnp.float32) for _ in range(bin_tiles))
    tables = lax.fori_loop(0, (last - first) // CHUNK + 1, some_bins, start)
    for q, table in enumerate(tables):
        table_ref[q * SUBS : (q + 1) * SUBS, :] = table


def level_kernel(
    groups, integrations, bin_tiles, margin, gain_ref, bins_ref, own_ref, next_ref, rim_ref, factor_ref, edge_ref
):
    cols = gain_ref.shape[0]
    tiles = cols // SUBS
    lane, row = lane_iota(), row_iota()
    section_first = lax.axis_index("section") * groups
    at_end = lax.axis_index("freq") == lax.axis_size("freq") - 1
    inverse = []
    for q in range(bin_tiles):
        stacked = jnp.zeros((SUBS, LANES), jnp.float32)
        for side, ref in enumerate((own_ref, next_ref)):
            rows = [ref[q * SUBS + r : q * SUBS + r + 1, :] for r in range(groups + 2)]
            running = rows[groups + 1]
            for group in range(groups):
                running = running + rows[group]
                tally = rows[groups] * ((section_first + group + 1) * integrations).astype(jnp.float32)
                stacked = jnp.where(row == side * groups + group, tally / running, stacked)
        inverse.append(stacked)
    bins = [row_tile(bins_ref, 0, tile, tiles) for tile in range(tiles)]
    rim_row = groups * integrations
    rim_bins = rim_ref[rim_row : rim_row + SUBS, :].astype(jnp.int32)
    first, last = jnp.min(bins[0]), jnp.max(bins[-1])
    rim_last = jnp.max(jnp.where((lane < margin) & jnp.logical_not(at_end), rim_bins, 0))
    last = jnp.maximum(last, rim_last)

    def some_bins(step, found):
        found = list(found)
        for u in range(CHUNK):
            b = first + step * CHUNK + u
            picked = jnp.zeros((SUBS, LANES), jnp.float32)
            for q in range(bin_tiles):
                picked = jnp.where(lane == b - q * LANES, inverse[q], picked)
            level = jnp.sum(picked, axis=1, keepdims=True)
            for tile in range(tiles + 1):
                mask = (bins[tile] if tile < tiles else rim_bins) == b
                for group in range(groups):
                    at = group * (tiles + 1) + tile
                    source = group if tile < tiles else groups + group
                    found[at] = jnp.where(mask, level[source : source + 1, :], found[at])
        return tuple(found)

    start = tuple(jnp.zeros((SUBS, LANES), jnp.float32) for _ in range(groups * (tiles + 1)))
    found = lax.fori_loop(0, (last - first) // CHUNK + 1, some_bins, start)
    for group in range(groups):
        for tile in range(tiles):
            factor_ref[pl.ds((group * tiles + tile) * SUBS, SUBS), :] = found[
                group * (tiles + 1) + tile
            ] * row_tile(gain_ref, 0, tile, tiles)
        for block in range(integrations // SUBS):
            at = (group * (integrations // SUBS) + block) * SUBS
            normal = rim_ref[at : at + SUBS, :] * found[group * (tiles + 1) + tiles] - 1.0
            edge_ref[at : at + SUBS, :] = jnp.where(at_end, 0.0, normal)


def tree_kernel(
    groups, integrations, strides, hop, x_ref, factor_ref, edge_ref, cut_ref, reach_ref, out_ref
):
    rows_out = out_ref.shape[0] // (groups * strides)
    cols = rows_out
    tiles = cols // SUBS
    lane, row = lane_iota(), row_iota()
    section = lax.axis_index("section")
    target = lax.rem(section + hop, lax.axis_size("section"))

    def one_row(group, t, tile):
        block = spectra_tile(x_ref, group, t, tile % tiles, cols, integrations)
        at = (group * tiles + tile % tiles) * SUBS
        normal = block * factor_ref[at : at + SUBS, :] - 1.0
        if tile < tiles:
            return normal
        at = group * integrations + t
        return jnp.where(row == SUBS - 1, edge_ref[at : at + 1, :], pltpu.roll(normal, SUBS - 1, 0))

    def one_stride(group, index, stride):
        def moved(here, there, steps):
            if steps == 0:
                return here
            if there is not None:
                here = jnp.where(lane < steps * stride, there, here)
            return pltpu.roll(here, LANES - steps * stride, 1)

        group_id = section * groups + group
        later = {}
        for tile in range(tiles, -1, -1):

            def merge(level, block):
                if level == 0:
                    return [one_row(group, block, tile)]
                former = merge(level - 1, 2 * block)
                latter = merge(level - 1, 2 * block + 1)
                result = []
                for half, (anchor, source) in enumerate(zip(former, latter)):
                    beyond = later.get((level, block, half))
                    later[(level, block, half)] = source
                    result.append(anchor + moved(source, beyond, half))
                    result.append(anchor + moved(source, beyond, half + 1))
                return result

            final = merge(integrations.bit_length() - 1, 0)
            if tile == tiles:
                continue
            score = jnp.zeros((SUBS, LANES), jnp.float32)
            for drift, value in enumerate(final):
                cut = cut_ref[group_id, stride - 1, drift].astype(jnp.float32) * (4.0 / 256.0)
                score = score + jnp.maximum(value - cut, 0.0)
            at = (group * strides + index) * cols + tile
            out_ref[pl.ds(at, SUBS, stride=tiles), :] = score * (0.25 / integrations)

    for group in range(groups):
        for index in range(strides):
            stride = target * strides + index + 1
            reached = stride <= reach_ref[section * groups + group]

            @pl.when(reached)
            def _():
                one_stride(group, index, stride)

            @pl.when(jnp.logical_not(reached))
            def _():
                at = (group * strides + index) * cols
                out_ref[at : at + cols, :] = jnp.zeros((cols, LANES), jnp.float32)


def swap(value, partner):
    sections, freqs = lax.axis_size("section"), lax.axis_size("freq")
    route = []
    for section in range(sections):
        for freq in range(freqs):
            to_section, to_freq = partner(section, freq)
            route.append((section * freqs + freq, to_section * freqs + to_freq))
    return lax.ppermute(value, BOTH, route)


def shards(spectra, channel_gain, bandpass_bin, drift_range, hit_cutoff):
    groups, integrations, chan_dev = spectra.shape
    sections, freqs = lax.axis_size("section"), lax.axis_size("freq")
    section, freq = lax.axis_index("section"), lax.axis_index("freq")
    total_bins = 4 * freqs
    bin_tiles = -(-total_bins // LANES)
    rates = hit_cutoff.shape[1]
    strides = rates // sections
    margin = rates * (integrations - 1)
    cols = chan_dev // LANES
    blocks = integrations // SUBS
    assert cols % SUBS == 0 and integrations % SUBS == 0 and margin <= LANES
    assert freqs % 2 == 0 and 2 * groups <= SUBS and groups + 2 <= SUBS and rates % sections == 0
    x = spectra.reshape(groups, blocks, SUBS, cols, LANES).transpose(0, 1, 3, 2, 4)
    x = x.reshape(groups * blocks * cols * SUBS, LANES)
    gain = channel_gain.reshape(cols, LANES)
    bins = bandpass_bin.reshape(cols, LANES)
    rim_rows = groups * integrations
    shape = functools.partial(jax.ShapeDtypeStruct, dtype=jnp.float32)

    table, rim = pl.pallas_call(
        functools.partial(bin_kernel, groups, integrations, bin_tiles),
        out_shape=(shape((bin_tiles * SUBS, LANES)), shape((rim_rows + SUBS, LANES))),
        in_specs=[VMEM] * 3,
        out_specs=(VMEM, VMEM),
        compiler_params=PARAMS,
        name="bin_sums",
    )(x, gain, bins)

    row_kind = lax.broadcasted_iota(jnp.int32, table.shape, 0) % SUBS

    def group_total(value):
        parts = value.reshape(bin_tiles, SUBS, LANES)[:, :groups]
        total = jnp.sum(parts, axis=1, keepdims=True)
        return jnp.broadcast_to(total, (bin_tiles, SUBS, LANES)).reshape(value.shape)

    if sections == 2:
        before = group_total(swap(table, lambda s, f: (1 - s, f)))
        before = jnp.where(section == 1, before, 0.0)
    else:
        all_tables = lax.all_gather(table, "section")
        earlier = lax.broadcasted_iota(jnp.int32, (sections, 1, 1), 0) < section
        before = group_total(jnp.sum(jnp.where(earlier, all_tables, 0.0), axis=0))
    table = jnp.where(row_kind == groups + 1, before, table)

    mate = lambda s, f: (s, f ^ 1)

    def across(s, f):
        other = f + 1 if f % 2 else f - 1
        if 0 <= other < freqs:
            return (s, other)
        return (s ^ 1, f) if sections % 2 == 0 else (s, f)

    packed = jnp.concatenate([table, rim], axis=0)
    from_mate = swap(packed, mate)
    rows = table.shape[0]
    pair = table + from_mate[:rows]
    from_across = swap(jnp.concatenate([pair, rim], axis=0), across)
    has_across = jnp.logical_and(freq != 0, freq != freqs - 1)
    own = pair + jnp.where(has_across, from_across[:rows], 0.0)
    odd = freq % 2 == 1
    following = jnp.where(odd, own, swap(own, mate))
    next_rim = jnp.where(odd, from_across[rows:], from_mate[rows:])

    factor, edge = pl.pallas_call(
        functools.partial(level_kernel, groups, integrations, bin_tiles, margin),
        out_shape=(shape((groups * cols, LANES)), shape((rim_rows, LANES))),
        in_specs=[VMEM] * 5,
        out_specs=(VMEM, VMEM),
        compiler_params=PARAMS,
        name="levels",
    )(gain, bins, own, following, next_rim)

    def scores(hop):
        flops = 150 * groups * strides * integrations * chan_dev
        return pl.pallas_call(
            functools.partial(tree_kernel, groups, integrations, strides, hop),
            out_shape=shape((groups * strides * cols, LANES)),
            in_specs=[VMEM] * 3 + [SMEM] * 2,
            out_specs=VMEM,
            compiler_params=PARAMS,
            cost_estimate=pl.CostEstimate(flops=flops, bytes_accessed=0, transcendentals=0),
            name="tree",
        )(x, factor, edge, hit_cutoff, drift_range)

    arrived = []
    for hop in range(1, sections):
        arrived.append(swap(scores(hop), lambda s, f: ((s + hop) % sections, f)))
    parts = [scores(0)] + arrived
    if sections == 2:
        low, high = (jnp.where(section == 0, parts[i], parts[1 - i]) for i in (0, 1))
        out = jnp.concatenate([low, high], axis=0)
    else:
        out = jnp.zeros((sections,) + parts[0].shape, jnp.float32)
        for hop, part in enumerate(parts):
            out = lax.dynamic_update_index_in_dim(out, part, (section + sections - hop) % sections, 0)
    return out.reshape(sections * groups, strides, chan_dev)


def solution(mesh):
    return jax.shard_map(
        shards,
        mesh=mesh,
        in_specs=(P("section", None, "freq"), P("freq"), P("freq"), P(), P()),
        out_specs=P(None, "section", "freq"),
        check_vma=False,
    )
```

```python
import functools

import jax
import jax.numpy as jnp
from jax import lax
from jax.experimental import pallas as pl
from jax.experimental.pallas import tpu as pltpu
from jax.sharding import PartitionSpec as P

LANES = 128
SUBS = 8
BOTH = ("section", "freq")
CHUNK = 8
NEVER = 3e38
VMEM = pl.BlockSpec(memory_space=pltpu.VMEM)
SMEM = pl.BlockSpec(memory_space=pltpu.SMEM)
ANY = pl.BlockSpec(memory_space=pl.ANY)
PARAMS = pltpu.CompilerParams(vmem_limit_bytes=16 * 2**20)


def lane_iota():
    return lax.broadcasted_iota(jnp.int32, (SUBS, LANES), 1)


def row_iota():
    return lax.broadcasted_iota(jnp.int32, (SUBS, LANES), 0)


def spectra_rows(x_ref, group, t, first, rows, cols, integrations):
    block = group * (integrations // SUBS) + t // SUBS
    return x_ref[pl.ds((block * cols + first) * SUBS + t % SUBS, rows, stride=SUBS), :]


def bin_kernel(
    groups, integrations, bin_tiles, x_hbm, gain_hbm, bins_hbm, table_ref, rim_ref, x_ref, gain_ref, bins_ref, sems
):
    cols = gain_ref.shape[0]
    tiles = cols // SUBS
    group_rows = integrations * cols
    copies = [
        pltpu.make_async_copy(gain_hbm, gain_ref, sems.at[0]),
        pltpu.make_async_copy(bins_hbm, bins_ref, sems.at[1]),
    ]
    for group in range(groups):
        part = pl.ds(group * group_rows, group_rows)
        copies.append(pltpu.make_async_copy(x_hbm.at[part], x_ref.at[part], sems.at[2 + group]))
    for copy in copies:
        copy.start()
    lane, row = lane_iota(), row_iota()
    copies[0].wait()
    copies[1].wait()
    bins = [bins_ref[tile * SUBS : (tile + 1) * SUBS, :] for tile in range(tiles)]
    first, last = jnp.min(bins[0]), jnp.max(bins[-1])
    last_rows = groups * integrations
    rim_ref[last_rows : last_rows + SUBS, :] = jnp.broadcast_to(
        bins_ref[0:1, :].astype(jnp.float32), (SUBS, LANES)
    )
    summed = []
    for group in range(groups):
        copies[2 + group].wait()
        for block in range(integrations // SUBS):
            at = group * (integrations // SUBS) + block
            rim_ref[at * SUBS : (at + 1) * SUBS, :] = (
                x_ref[at * cols * SUBS : at * cols * SUBS + SUBS, :] * gain_ref[0:1, :]
            )
        for tile in range(tiles):
            parts = [
                spectra_rows(x_ref, group, t, tile * SUBS, SUBS, cols, integrations)
                for t in range(integrations)
            ]
            while len(parts) > 1:
                parts = [a + b for a, b in zip(parts[0::2], parts[1::2])]
            summed.append(parts[0] * gain_ref[tile * SUBS : (tile + 1) * SUBS, :])

    def some_bins(step, tables):
        for u in range(CHUNK):
            b = first + step * CHUNK + u
            masks = [part == b for part in bins]
            stacked = jnp.zeros((SUBS, LANES), jnp.float32)
            for quantity in range(groups + 1):
                partial = jnp.zeros((SUBS, LANES), jnp.float32)
                for tile in range(tiles):
                    value = 1.0 if quantity == groups else summed[quantity * tiles + tile]
                    partial = partial + jnp.where(masks[tile], value, 0.0)
                stacked = jnp.where(row == quantity, jnp.sum(partial, axis=0, keepdims=True), stacked)
            total = jnp.sum(stacked, axis=1, keepdims=True)
            tables = tuple(
                table + jnp.where(lane == b - q * LANES, total, 0.0) for q, table in enumerate(tables)
            )
        return tables

    start = tuple(jnp.zeros((SUBS, LANES), jnp.float32) for _ in range(bin_tiles))
    tables = lax.fori_loop(0, (last - first) // CHUNK + 1, some_bins, start)
    for q, table in enumerate(tables):
        table_ref[q * SUBS : (q + 1) * SUBS, :] = table


def turn_kernel(groups, integrations, x_ref, cut_ref, reach_ref, turned_ref, cuts_ref):
    cols = LANES // groups
    for t in range(integrations):
        block = jnp.concatenate(
            [spectra_rows(x_ref, group, t, 0, cols, cols, integrations) for group in range(groups)], axis=0
        )
        turned_ref[t * LANES : (t + 1) * LANES, :] = block.T
    lane = lax.broadcasted_iota(jnp.int32, (1, LANES), 1)
    section = lax.axis_index("section")
    for index in range(cut_ref.shape[1]):
        for drift in range(integrations):
            line = jnp.zeros((1, LANES), jnp.float32)
            for group in range(groups):
                group_id = section * groups + group
                cut = cut_ref[group_id, index, drift].astype(jnp.float32) * (4.0 / 256.0)
                cut = jnp.where(index + 1 <= reach_ref[group_id], cut, NEVER)
                line = jnp.where(lane // cols == group, cut, line)
            at = index * integrations + drift
            cuts_ref[at : at + 1, :] = line


def level_kernel(
    groups, integrations, bin_tiles, margin, span, gain_ref, bins_ref, own_ref, next_ref, rim_ref, turned_ref, normal_ref
):
    cols = gain_ref.shape[0]
    tiles = cols // SUBS
    lane, row = lane_iota(), row_iota()
    section_first = lax.axis_index("section") * groups
    at_end = lax.axis_index("freq") == lax.axis_size("freq") - 1
    inverse = []
    for q in range(bin_tiles):
        stacked = jnp.zeros((SUBS, LANES), jnp.float32)
        for side, ref in enumerate((own_ref, next_ref)):
            rows = [ref[q * SUBS + r : q * SUBS + r + 1, :] for r in range(groups + 2)]
            running = rows[groups + 1]
            for group in range(groups):
                running = running + rows[group]
                tally = rows[groups] * ((section_first + group + 1) * integrations).astype(jnp.float32)
                stacked = jnp.where(row == side * groups + group, tally / running, stacked)
        inverse.append(stacked)
    bins = [bins_ref[tile * SUBS : (tile + 1) * SUBS, :] for tile in range(tiles)]
    rim_row = groups * integrations
    rim_bins = rim_ref[rim_row : rim_row + SUBS, :].astype(jnp.int32)
    first, last = jnp.min(bins[0]), jnp.max(bins[-1])
    rim_last = jnp.max(jnp.where((lane < margin) & jnp.logical_not(at_end), rim_bins, 0))
    last = jnp.maximum(last, rim_last)

    def some_bins(step, found):
        found = list(found)
        for u in range(CHUNK):
            b = first + step * CHUNK + u
            picked = jnp.zeros((SUBS, LANES), jnp.float32)
            for q in range(bin_tiles):
                picked = jnp.where(lane == b - q * LANES, inverse[q], picked)
            level = jnp.sum(picked, axis=1, keepdims=True)
            for tile in range(tiles + 1):
                mask = (bins[tile] if tile < tiles else rim_bins) == b
                for group in range(groups):
                    at = group * (tiles + 1) + tile
                    source = group if tile < tiles else groups + group
                    found[at] = jnp.where(mask, level[source : source + 1, :], found[at])
        return tuple(found)

    start = tuple(jnp.zeros((SUBS, LANES), jnp.float32) for _ in range(groups * (tiles + 1)))
    found = lax.fori_loop(0, (last - first) // CHUNK + 1, some_bins, start)
    factors, rims = [], []
    for group in range(groups):
        for tile in range(tiles):
            factors.append(
                found[group * (tiles + 1) + tile] * gain_ref[tile * SUBS : (tile + 1) * SUBS, :]
            )
        for block in range(integrations // SUBS):
            at = (group * (integrations // SUBS) + block) * SUBS
            edge = rim_ref[at : at + SUBS, :] * found[group * (tiles + 1) + tiles] - 1.0
            rims.append(jnp.where(at_end, 0.0, edge))
        rims.append(jnp.zeros((cols - integrations, LANES), jnp.float32))
    factor = jnp.concatenate(factors, axis=0).T
    edges = jnp.concatenate(rims, axis=0).T
    extra = span - LANES
    lanes = lax.broadcasted_iota(jnp.int32, (extra, LANES), 1)
    for t in range(integrations):
        normal = turned_ref[t * LANES : (t + 1) * LANES, :] * factor - 1.0
        normal_ref[t * span : t * span + LANES, :] = normal
        inner = pltpu.roll(normal[:extra], LANES - 1, 1)
        outer = edges[:extra]
        if cols - 1 - t:
            outer = pltpu.roll(outer, cols - 1 - t, 1)
        normal_ref[t * span + LANES : (t + 1) * span, :] = jnp.where(
            lanes % cols == cols - 1, outer, inner
        )


def tree_kernel(groups, integrations, strides, rates, hop, span, normal_ref, cuts_ref, out_ref, *later_refs):
    levels = integrations.bit_length() - 1
    section = lax.axis_index("section")
    target = lax.rem(section + hop, lax.axis_size("section"))

    def values(level, block, at, stride):
        if level == 0:
            return [normal_ref[block * span + at : block * span + at + SUBS, :]]
        former = values(level - 1, 2 * block, at, stride)
        rows = 2 ** (level - 1)
        result = []
        for half, anchor in enumerate(former):
            if level == 1:
                ref, base = normal_ref, (2 * block + 1) * span
            else:
                ref, base = later_refs[level - 2], (block * rows + half) * span
            for steps in (half, half + 1):
                where = base + at + steps * stride
                result.append(anchor + ref[pl.ds(where, SUBS), :])
        return result

    for index in range(strides):
        stride = target * strides + index + 1
        for level in range(1, levels):
            reach = min(span, LANES + -(-(integrations - 2**level) * rates // SUBS) * SUBS)
            for block in range(1, integrations >> level, 2):
                for at in range(0, reach, SUBS):
                    for drift, value in enumerate(values(level, block, at, stride)):
                        row = ((block // 2) * 2**level + drift) * span + at
                        later_refs[level - 1][row : row + SUBS, :] = value
        parts = []
        for at in range(0, LANES, SUBS):
            score = jnp.zeros((SUBS, LANES), jnp.float32)
            for drift, value in enumerate(values(levels, 0, at, stride)):
                cut = cuts_ref[pl.ds((stride - 1) * integrations + drift, 1), :]
                score = score + jnp.maximum(value - cut, 0.0)
            parts.append(score * (0.25 / integrations))
        scores = jnp.concatenate(parts, axis=0).T
        cols = LANES // groups
        for group in range(groups):
            at = (group * strides + index) * cols
            out_ref[at : at + cols, :] = scores[group * cols : (group + 1) * cols]


def swap(value, partner):
    sections, freqs = lax.axis_size("section"), lax.axis_size("freq")
    route = []
    for section in range(sections):
        for freq in range(freqs):
            to_section, to_freq = partner(section, freq)
            route.append((section * freqs + freq, to_section * freqs + to_freq))
    return lax.ppermute(value, BOTH, route)


def shards(spectra, channel_gain, bandpass_bin, drift_range, hit_cutoff):
    groups, integrations, chan_dev = spectra.shape
    sections, freqs = lax.axis_size("section"), lax.axis_size("freq")
    section, freq = lax.axis_index("section"), lax.axis_index("freq")
    total_bins = 4 * freqs
    bin_tiles = -(-total_bins // LANES)
    rates = hit_cutoff.shape[1]
    strides = rates // sections
    margin = rates * (integrations - 1)
    cols = chan_dev // LANES
    blocks = integrations // SUBS
    assert cols % SUBS == 0 and integrations % SUBS == 0 and margin <= LANES - SUBS
    assert groups * cols == LANES and integrations <= cols
    assert freqs % 2 == 0 and 2 * groups <= SUBS and groups + 2 <= SUBS and rates % sections == 0
    x = spectra.reshape(groups, blocks, SUBS, cols, LANES).transpose(0, 1, 3, 2, 4)
    x = x.reshape(groups * blocks * cols * SUBS, LANES)
    gain = channel_gain.reshape(cols, LANES)
    bins = bandpass_bin.reshape(cols, LANES)
    rim_rows = groups * integrations
    shape = functools.partial(jax.ShapeDtypeStruct, dtype=jnp.float32)

    table, rim = pl.pallas_call(
        functools.partial(bin_kernel, groups, integrations, bin_tiles),
        out_shape=(shape((bin_tiles * SUBS, LANES)), shape((rim_rows + SUBS, LANES))),
        in_specs=[ANY] * 3,
        out_specs=(VMEM, VMEM),
        scratch_shapes=[
            pltpu.VMEM(x.shape, jnp.float32),
            pltpu.VMEM(gain.shape, jnp.float32),
            pltpu.VMEM(bins.shape, jnp.int32),
            pltpu.SemaphoreType.DMA((2 + groups,)),
        ],
        compiler_params=PARAMS,
        name="bin_sums",
    )(x, gain, bins)

    turned, cuts = pl.pallas_call(
        functools.partial(turn_kernel, groups, integrations),
        out_shape=(shape((integrations * LANES, LANES)), shape((rates * integrations, LANES))),
        in_specs=[VMEM, SMEM, SMEM],
        out_specs=(VMEM, VMEM),
        compiler_params=PARAMS,
        cost_estimate=pl.CostEstimate(flops=10**7, bytes_accessed=0, transcendentals=0),
        name="turn",
    )(x, hit_cutoff, drift_range)

    row_kind = lax.broadcasted_iota(jnp.int32, table.shape, 0) % SUBS

    def group_total(value):
        parts = value.reshape(bin_tiles, SUBS, LANES)[:, :groups]
        total = jnp.sum(parts, axis=1, keepdims=True)
        return jnp.broadcast_to(total, (bin_tiles, SUBS, LANES)).reshape(value.shape)

    if sections == 2:
        before = group_total(swap(table, lambda s, f: (1 - s, f)))
        before = jnp.where(section == 1, before, 0.0)
    else:
        all_tables = lax.all_gather(table, "section")
        earlier = lax.broadcasted_iota(jnp.int32, (sections, 1, 1), 0) < section
        before = group_total(jnp.sum(jnp.where(earlier, all_tables, 0.0), axis=0))
    table = jnp.where(row_kind == groups + 1, before, table)

    mate = lambda s, f: (s, f ^ 1)

    def across(s, f):
        other = f + 1 if f % 2 else f - 1
        if 0 <= other < freqs:
            return (s, other)
        return (s ^ 1, f) if sections % 2 == 0 else (s, f)

    packed = jnp.concatenate([table, rim], axis=0)
    from_mate = swap(packed, mate)
    rows = table.shape[0]
    pair = table + from_mate[:rows]
    from_across = swap(jnp.concatenate([pair, rim], axis=0), across)
    has_across = jnp.logical_and(freq != 0, freq != freqs - 1)
    own = pair + jnp.where(has_across, from_across[:rows], 0.0)
    odd = freq % 2 == 1
    following = jnp.where(odd, own, swap(own, mate))
    next_rim = jnp.where(odd, from_across[rows:], from_mate[rows:])

    span = LANES + -(-margin // SUBS) * SUBS + SUBS
    normal = pl.pallas_call(
        functools.partial(level_kernel, groups, integrations, bin_tiles, margin, span),
        out_shape=shape((integrations * span, LANES)),
        in_specs=[VMEM] * 6,
        out_specs=VMEM,
        compiler_params=PARAMS,
        name="levels",
    )(gain, bins, own, following, next_rim, turned)

    def scores(hop):
        flops = 150 * groups * strides * integrations * chan_dev
        later = pltpu.VMEM((integrations // 2 * span, LANES), jnp.float32)
        return pl.pallas_call(
            functools.partial(tree_kernel, groups, integrations, strides, rates, hop, span),
            out_shape=shape((groups * strides * cols, LANES)),
            in_specs=[VMEM] * 2,
            out_specs=VMEM,
            scratch_shapes=[later] * (integrations.bit_length() - 2),
            compiler_params=PARAMS,
            cost_estimate=pl.CostEstimate(flops=flops, bytes_accessed=0, transcendentals=0),
            name="tree",
        )(normal, cuts)

    arrived = []
    for hop in range(1, sections):
        arrived.append(swap(scores(hop), lambda s, f: ((s + hop) % sections, f)))
    parts = [scores(0)] + arrived
    if sections == 2:
        low, high = (jnp.where(section == 0, parts[i], parts[1 - i]) for i in (0, 1))
        out = jnp.concatenate([low, high], axis=0)
    else:
        out = jnp.zeros((sections,) + parts[0].shape, jnp.float32)
        for hop, part in enumerate(parts):
            out = lax.dynamic_update_index_in_dim(out, part, (section + sections - hop) % sections, 0)
    return out.reshape(sections * groups, strides, chan_dev)


def solution(mesh):
    return jax.shard_map(
        shards,
        mesh=mesh,
        in_specs=(P("section", None, "freq"), P("freq"), P("freq"), P(), P()),
        out_specs=P(None, "section", "freq"),
        check_vma=False,
    )
```

```python
import functools

import jax
import jax.numpy as jnp
from jax import lax
from jax.experimental import pallas as pl
from jax.experimental.pallas import tpu as pltpu
from jax.sharding import PartitionSpec as P

LANES = 128
SUBS = 8
BOTH = ("section", "freq")
CHUNK = 8
NEVER = 3e38
VMEM = pl.BlockSpec(memory_space=pltpu.VMEM)
SMEM = pl.BlockSpec(memory_space=pltpu.SMEM)
HBM = pl.BlockSpec(memory_space=pltpu.HBM)
PARAMS = pltpu.CompilerParams(vmem_limit_bytes=16 * 2**20)


def lane_iota():
    return lax.broadcasted_iota(jnp.int32, (SUBS, LANES), 1)


def row_iota():
    return lax.broadcasted_iota(jnp.int32, (SUBS, LANES), 0)


def spectra_rows(x_ref, group, t, first, rows, cols, integrations):
    block = group * (integrations // SUBS) + t // SUBS
    return x_ref[pl.ds((block * cols + first) * SUBS + t % SUBS, rows, stride=SUBS), :]


def pack_count(margin):
    room = 1 << (margin - 1).bit_length()
    return LANES // room, room


def bin_kernel(
    groups,
    integrations,
    bin_tiles,
    margin,
    x_hbm,
    gain_hbm,
    bins_hbm,
    table_ref,
    shifted_ref,
    rim_ref,
    x_ref,
    gain_ref,
    bins_ref,
    sems,
):
    cols = gain_ref.shape[0]
    tiles = cols // SUBS
    group_rows = integrations * cols
    copies = [
        pltpu.make_async_copy(bins_hbm, bins_ref, sems.at[0]),
        pltpu.make_async_copy(gain_hbm, gain_ref, sems.at[1]),
    ]
    for group in range(groups):
        part = pl.ds(group * group_rows, group_rows)
        copies.append(pltpu.make_async_copy(x_hbm.at[part], x_ref.at[part], sems.at[2 + group]))
    for copy in copies:
        copy.start()
    lane, row = lane_iota(), row_iota()
    copies[0].wait()
    bins = [bins_ref[tile * SUBS : (tile + 1) * SUBS, :] for tile in range(tiles)]
    first, last = jnp.min(bins[0]), jnp.max(bins[-1])
    copies[1].wait()
    summed, rims = [], []
    for group in range(groups):
        copies[2 + group].wait()
        for block in range(integrations // SUBS):
            at = (group * (integrations // SUBS) + block) * cols * SUBS
            rims.append(x_ref[at : at + SUBS, :] * gain_ref[0:1, :])
        for tile in range(tiles):
            parts = [
                spectra_rows(x_ref, group, t, tile * SUBS, SUBS, cols, integrations)
                for t in range(integrations)
            ]
            while len(parts) > 1:
                parts = [a + b for a, b in zip(parts[0::2], parts[1::2])]
            summed.append(parts[0] * gain_ref[tile * SUBS : (tile + 1) * SUBS, :])
    side, room = pack_count(margin)
    for at in range(0, len(rims), side):
        packed = rims[at]
        for place, rim in enumerate(rims[at + 1 : at + side], 1):
            packed = jnp.where(lane // room == place, pltpu.roll(rim, place * room, 1), packed)
        rim_ref[at // side * SUBS : (at // side + 1) * SUBS, :] = packed

    def some_bins(step, tables):
        for u in range(CHUNK):
            b = first + step * CHUNK + u
            masks = [part == b for part in bins]
            stacked = jnp.zeros((SUBS, LANES), jnp.float32)
            for quantity in range(groups + 1):
                partial = jnp.zeros((SUBS, LANES), jnp.float32)
                for tile in range(tiles):
                    value = 1.0 if quantity == groups else summed[quantity * tiles + tile]
                    partial = partial + jnp.where(masks[tile], value, 0.0)
                stacked = jnp.where(row == quantity, jnp.sum(partial, axis=0, keepdims=True), stacked)
            total = jnp.sum(stacked, axis=1, keepdims=True)
            tables = tuple(
                table + jnp.where(lane == b - q * LANES, total, 0.0) for q, table in enumerate(tables)
            )
        return tables

    start = tuple(jnp.zeros((SUBS, LANES), jnp.float32) for _ in range(bin_tiles))
    tables = lax.fori_loop(0, (last - first) // CHUNK + 1, some_bins, start)
    rim_bins = jnp.broadcast_to(bins_ref[0:1, :].astype(jnp.float32), (SUBS, LANES))
    rim_bins_row = SUBS - 2 + lax.rem(lax.axis_index("freq"), 2)
    for q, table in enumerate(tables):
        shifted = pltpu.roll(table, groups + 1, 0)
        shifted_ref[q * SUBS : (q + 1) * SUBS, :] = jnp.where(
            (row > groups) & (row <= 2 * groups), shifted, 0.0
        )
        if q == 0:
            table = jnp.where(row == rim_bins_row, rim_bins, table)
        table_ref[q * SUBS : (q + 1) * SUBS, :] = table


def turn_kernel(groups, integrations, x_ref, cut_hbm, reach_hbm, turned_ref, cuts_ref, cut_ref, reach_ref, sems):
    copies = [
        pltpu.make_async_copy(cut_hbm, cut_ref, sems.at[0]),
        pltpu.make_async_copy(reach_hbm, reach_ref, sems.at[1]),
    ]
    for copy in copies:
        copy.start()
    cols = LANES // groups
    for t in range(integrations):
        block = jnp.concatenate(
            [spectra_rows(x_ref, group, t, 0, cols, cols, integrations) for group in range(groups)], axis=0
        )
        turned_ref[t * LANES : (t + 1) * LANES, :] = block.T
    for copy in copies:
        copy.wait()
    lane = lax.broadcasted_iota(jnp.int32, (1, LANES), 1)
    section = lax.axis_index("section")
    for index in range(cut_ref.shape[1]):
        for drift in range(integrations):
            line = jnp.zeros((1, LANES), jnp.float32)
            for group in range(groups):
                group_id = section * groups + group
                cut = cut_ref[group_id, index, drift].astype(jnp.float32) * (4.0 / 256.0)
                cut = jnp.where(index + 1 <= reach_ref[group_id], cut, NEVER)
                line = jnp.where(lane // cols == group, cut, line)
            at = index * integrations + drift
            cuts_ref[at : at + 1, :] = line


def level_kernel(
    groups,
    integrations,
    bin_tiles,
    margin,
    span,
    gain_ref,
    bins_ref,
    own_ref,
    next_ref,
    rim_bins_ref,
    rim_ref,
    turned_ref,
    normal_ref,
):
    cols = gain_ref.shape[0]
    tiles = cols // SUBS
    lane, row = lane_iota(), row_iota()
    section_first = lax.axis_index("section") * groups
    at_end = lax.axis_index("freq") == lax.axis_size("freq") - 1
    inverse = []
    for q in range(bin_tiles):
        stacked = jnp.zeros((SUBS, LANES), jnp.float32)
        for side, ref in enumerate((own_ref, next_ref)):
            rows = [ref[q * SUBS + r : q * SUBS + r + 1, :] for r in range(2 * groups + 1)]
            running = sum(rows[groups + 2 :], rows[groups + 1])
            for group in range(groups):
                running = running + rows[group]
                tally = rows[groups] * ((section_first + group + 1) * integrations).astype(jnp.float32)
                stacked = jnp.where(row == side * groups + group, tally / running, stacked)
        inverse.append(stacked)
    bins = [bins_ref[tile * SUBS : (tile + 1) * SUBS, :] for tile in range(tiles)]
    rim_bins = jnp.broadcast_to(rim_bins_ref[0:1, :], (SUBS, LANES)).astype(jnp.int32)
    first, last = jnp.min(bins[0]), jnp.max(bins[-1])
    rim_last = jnp.max(jnp.where((lane < margin) & jnp.logical_not(at_end), rim_bins, 0))
    last = jnp.maximum(last, rim_last)

    def some_bins(step, found):
        found = list(found)
        for u in range(CHUNK):
            b = first + step * CHUNK + u
            picked = jnp.zeros((SUBS, LANES), jnp.float32)
            for q in range(bin_tiles):
                picked = jnp.where(lane == b - q * LANES, inverse[q], picked)
            level = jnp.sum(picked, axis=1, keepdims=True)
            for tile in range(tiles + 1):
                mask = (bins[tile] if tile < tiles else rim_bins) == b
                for group in range(groups):
                    at = group * (tiles + 1) + tile
                    source = group if tile < tiles else groups + group
                    found[at] = jnp.where(mask, level[source : source + 1, :], found[at])
        return tuple(found)

    start = tuple(jnp.zeros((SUBS, LANES), jnp.float32) for _ in range(groups * (tiles + 1)))
    found = lax.fori_loop(0, (last - first) // CHUNK + 1, some_bins, start)
    factors, rims = [], []
    side, room = pack_count(margin)
    for group in range(groups):
        for tile in range(tiles):
            factors.append(
                found[group * (tiles + 1) + tile] * gain_ref[tile * SUBS : (tile + 1) * SUBS, :]
            )
        for block in range(integrations // SUBS):
            at = group * (integrations // SUBS) + block
            rim = rim_ref[at // side * SUBS : (at // side + 1) * SUBS, :]
            if at % side:
                rim = pltpu.roll(rim, LANES - at % side * room, 1)
            edge = rim * found[group * (tiles + 1) + tiles] - 1.0
            rims.append(jnp.where(at_end, 0.0, edge))
        rims.append(jnp.zeros((cols - integrations, LANES), jnp.float32))
    factor = jnp.concatenate(factors, axis=0).T
    edges = jnp.concatenate(rims, axis=0).T
    extra = span - LANES
    lanes = lax.broadcasted_iota(jnp.int32, (extra, LANES), 1)
    for t in range(integrations):
        normal = turned_ref[t * LANES : (t + 1) * LANES, :] * factor - 1.0
        normal_ref[t * span : t * span + LANES, :] = normal
        inner = pltpu.roll(normal[:extra], LANES - 1, 1)
        outer = edges[:extra]
        if cols - 1 - t:
            outer = pltpu.roll(outer, cols - 1 - t, 1)
        normal_ref[t * span + LANES : (t + 1) * span, :] = jnp.where(
            lanes % cols == cols - 1, outer, inner
        )


def tree_kernel(groups, integrations, strides, rates, hop, span, normal_ref, cuts_ref, out_ref, *later_refs):
    levels = integrations.bit_length() - 1
    section = lax.axis_index("section")
    target = lax.rem(section + hop, lax.axis_size("section"))

    def values(level, block, at, stride):
        if level == 0:
            return [normal_ref[block * span + at : block * span + at + SUBS, :]]
        former = values(level - 1, 2 * block, at, stride)
        rows = 2 ** (level - 1)
        result = []
        for half, anchor in enumerate(former):
            if level == 1:
                ref, base = normal_ref, (2 * block + 1) * span
            else:
                ref, base = later_refs[level - 2], (block * rows + half) * span
            for steps in (half, half + 1):
                where = base + at + steps * stride
                result.append(anchor + ref[pl.ds(where, SUBS), :])
        return result

    for index in range(strides):
        stride = target * strides + index + 1
        for level in range(1, levels):
            reach = min(span, LANES + -(-(integrations - 2**level) * rates // SUBS) * SUBS)
            for block in range(1, integrations >> level, 2):
                for at in range(0, reach, SUBS):
                    for drift, value in enumerate(values(level, block, at, stride)):
                        row = ((block // 2) * 2**level + drift) * span + at
                        later_refs[level - 1][row : row + SUBS, :] = value
        parts = []
        for at in range(0, LANES, SUBS):
            score = jnp.zeros((SUBS, LANES), jnp.float32)
            for drift, value in enumerate(values(levels, 0, at, stride)):
                cut = cuts_ref[pl.ds((stride - 1) * integrations + drift, 1), :]
                score = score + jnp.maximum(value - cut, 0.0)
            parts.append(score * (0.25 / integrations))
        scores = jnp.concatenate(parts, axis=0).T
        cols = LANES // groups
        for group in range(groups):
            at = (group * strides + index) * cols
            out_ref[at : at + cols, :] = scores[group * cols : (group + 1) * cols]


def far(value):
    return pltpu.with_memory_space_constraint(value, pltpu.HBM)


def swap(value, partner):
    sections, freqs = lax.axis_size("section"), lax.axis_size("freq")
    route = []
    for section in range(sections):
        for freq in range(freqs):
            to_section, to_freq = partner(section, freq)
            route.append((section * freqs + freq, to_section * freqs + to_freq))
    return lax.ppermute(value, BOTH, route)


def shards(spectra, channel_gain, bandpass_bin, drift_range, hit_cutoff):
    groups, integrations, chan_dev = spectra.shape
    sections, freqs = lax.axis_size("section"), lax.axis_size("freq")
    section, freq = lax.axis_index("section"), lax.axis_index("freq")
    total_bins = 4 * freqs
    bin_tiles = -(-total_bins // LANES)
    rates = hit_cutoff.shape[1]
    strides = rates // sections
    margin = rates * (integrations - 1)
    cols = chan_dev // LANES
    blocks = integrations // SUBS
    assert cols % SUBS == 0 and integrations % SUBS == 0 and margin <= LANES - SUBS
    assert groups * cols == LANES and integrations <= cols
    assert freqs % 2 == 0 and 2 * groups + 1 <= SUBS - 2 and rates % sections == 0
    x = spectra.reshape(groups, blocks, SUBS, cols, LANES).transpose(0, 1, 3, 2, 4)
    x = x.reshape(groups * blocks * cols * SUBS, LANES)
    gain = channel_gain.reshape(cols, LANES)
    bins = bandpass_bin.reshape(cols, LANES)
    shape = functools.partial(jax.ShapeDtypeStruct, dtype=jnp.float32)
    side, _ = pack_count(margin)
    rim_tiles = -(-groups * blocks // side)

    table, shifted, rim, x_near, gain_near, bins_near = pl.pallas_call(
        functools.partial(bin_kernel, groups, integrations, bin_tiles, margin),
        out_shape=(
            shape((bin_tiles * SUBS, LANES)),
            shape((bin_tiles * SUBS, LANES)),
            shape((rim_tiles * SUBS, LANES)),
            shape(x.shape),
            shape(gain.shape),
            jax.ShapeDtypeStruct(bins.shape, bins.dtype),
        ),
        in_specs=[HBM] * 3,
        out_specs=(VMEM,) * 6,
        scratch_shapes=[pltpu.SemaphoreType.DMA((2 + groups,))],
        compiler_params=PARAMS,
        name="bin_sums",
    )(far(x), far(gain), far(bins))

    turned, cuts = pl.pallas_call(
        functools.partial(turn_kernel, groups, integrations),
        out_shape=(shape((integrations * LANES, LANES)), shape((rates * integrations, LANES))),
        in_specs=[VMEM, HBM, HBM],
        out_specs=(VMEM, VMEM),
        scratch_shapes=[
            pltpu.SMEM(hit_cutoff.shape, jnp.int32),
            pltpu.SMEM(drift_range.shape, jnp.int32),
            pltpu.SemaphoreType.DMA((2,)),
        ],
        compiler_params=PARAMS,
        cost_estimate=pl.CostEstimate(flops=10**7, bytes_accessed=0, transcendentals=0),
        name="turn",
    )(x_near, far(hit_cutoff), far(drift_range))

    mate = lambda s, f: (s, f ^ 1)

    def across(s, f):
        other = f + 1 if f % 2 else f - 1
        if 0 <= other < freqs:
            return (s, other)
        return (s ^ 1, f) if sections % 2 == 0 else (s, f)

    rows = table.shape[0]
    if sections == 2:
        level_here = swap(shifted, lambda s, f: (1 - s, f))
        level_mate = swap(shifted, lambda s, f: (1 - s, f ^ 1))
        from_mate = swap(jnp.concatenate([table, rim], axis=0), mate)
        earlier = jnp.where(section == 1, level_here + level_mate, 0.0)
        pair = table + from_mate[:rows] + earlier
    else:
        all_shifted = lax.all_gather(shifted, "section")
        is_earlier = lax.broadcasted_iota(jnp.int32, (sections, 1, 1), 0) < section
        table = table + jnp.sum(jnp.where(is_earlier, all_shifted, 0.0), axis=0)
        from_mate = swap(jnp.concatenate([table, rim], axis=0), mate)
        pair = table + from_mate[:rows]
    from_across = swap(jnp.concatenate([pair, rim], axis=0), across)
    has_across = jnp.logical_and(freq != 0, freq != freqs - 1)
    own = pair + jnp.where(has_across, from_across[:rows], 0.0)
    odd = freq % 2 == 1
    following = jnp.where(odd, own, swap(own, mate))
    next_rim = jnp.where(odd, from_across[rows:], from_mate[rows:])
    next_bins = jnp.where(odd, from_across[SUBS - 2 : SUBS - 1], from_mate[SUBS - 1 : SUBS])

    span = LANES + -(-margin // SUBS) * SUBS + SUBS
    normal = pl.pallas_call(
        functools.partial(level_kernel, groups, integrations, bin_tiles, margin, span),
        out_shape=shape((integrations * span, LANES)),
        in_specs=[VMEM] * 7,
        out_specs=VMEM,
        compiler_params=PARAMS,
        name="levels",
    )(gain_near, bins_near, own, following, next_bins, next_rim, turned)

    def scores(hop):
        flops = 150 * groups * strides * integrations * chan_dev
        later = pltpu.VMEM((integrations // 2 * span, LANES), jnp.float32)
        return pl.pallas_call(
            functools.partial(tree_kernel, groups, integrations, strides, rates, hop, span),
            out_shape=shape((groups * strides * cols, LANES)),
            in_specs=[VMEM] * 2,
            out_specs=VMEM,
            scratch_shapes=[later] * (integrations.bit_length() - 2),
            compiler_params=PARAMS,
            cost_estimate=pl.CostEstimate(flops=flops, bytes_accessed=0, transcendentals=0),
            name="tree",
        )(normal, cuts)

    arrived = []
    for hop in range(1, sections):
        arrived.append(swap(scores(hop), lambda s, f: ((s + hop) % sections, f)))
    parts = [scores(0)] + arrived
    if sections == 2:
        low, high = (jnp.where(section == 0, parts[i], parts[1 - i]) for i in (0, 1))
        out = jnp.concatenate([low, high], axis=0)
    else:
        out = jnp.zeros((sections,) + parts[0].shape, jnp.float32)
        for hop, part in enumerate(parts):
            out = lax.dynamic_update_index_in_dim(out, part, (section + sections - hop) % sections, 0)
    return out.reshape(sections * groups, strides, chan_dev)


def solution(mesh):
    return jax.shard_map(
        shards,
        mesh=mesh,
        in_specs=(P("section", None, "freq"), P("freq"), P("freq"), P(), P()),
        out_specs=P(None, "section", "freq"),
        check_vma=False,
    )
```

```python
import dataclasses
import functools

import jax
import jax.numpy as jnp
from jax import lax
from jax.experimental import pallas as pl
from jax.experimental.pallas import tpu as pltpu
from jax.sharding import PartitionSpec as P

LANES = 128
SUBS = 8
BOTH = ("section", "freq")
CHUNK = 8
NEVER = 3e38
VMEM = pl.BlockSpec(memory_space=pltpu.VMEM)
SMEM = pl.BlockSpec(memory_space=pltpu.SMEM)
HBM = pl.BlockSpec(memory_space=pltpu.HBM)
PARAMS = pltpu.CompilerParams(vmem_limit_bytes=16 * 2**20)


@dataclasses.dataclass(frozen=True)
class Sizes:
    groups: int
    integrations: int
    bin_tiles: int
    margin: int
    rates: int
    strides: int

    @property
    def extra(self):
        return -(-self.margin // SUBS) * SUBS + SUBS

    @property
    def head(self):
        return LANES - -(-self.margin // SUBS) * SUBS

    @property
    def main_span(self):
        return LANES + SUBS

    @property
    def tail_span(self):
        return LANES - self.head + self.extra


def lane_iota():
    return lax.broadcasted_iota(jnp.int32, (SUBS, LANES), 1)


def row_iota():
    return lax.broadcasted_iota(jnp.int32, (SUBS, LANES), 0)


def spectra_rows(x_ref, group, t, first, rows, cols, integrations):
    block = group * (integrations // SUBS) + t // SUBS
    return x_ref[pl.ds((block * cols + first) * SUBS + t % SUBS, rows, stride=SUBS), :]


def pack_count(margin):
    room = 1 << (margin - 1).bit_length()
    return LANES // room, room


def bin_kernel(
    groups,
    integrations,
    bin_tiles,
    margin,
    x_hbm,
    gain_hbm,
    bins_hbm,
    packed_ref,
    x_ref,
    gain_ref,
    bins_ref,
    sems,
):
    cols = gain_ref.shape[0]
    tiles = cols // SUBS
    group_rows = integrations * cols
    copies = [
        pltpu.make_async_copy(bins_hbm, bins_ref, sems.at[0]),
        pltpu.make_async_copy(gain_hbm, gain_ref, sems.at[1]),
    ]
    for group in range(groups):
        part = pl.ds(group * group_rows, group_rows)
        copies.append(pltpu.make_async_copy(x_hbm.at[part], x_ref.at[part], sems.at[2 + group]))
    for copy in copies:
        copy.start()
    lane, row = lane_iota(), row_iota()
    copies[0].wait()
    bins = [bins_ref[tile * SUBS : (tile + 1) * SUBS, :] for tile in range(tiles)]
    first, last = jnp.min(bins[0]), jnp.max(bins[-1])
    copies[1].wait()
    summed, rims = [], []
    for group in range(groups):
        copies[2 + group].wait()
        for block in range(integrations // SUBS):
            at = (group * (integrations // SUBS) + block) * cols * SUBS
            rims.append(x_ref[at : at + SUBS, :] * gain_ref[0:1, :])
        for tile in range(tiles):
            parts = [
                spectra_rows(x_ref, group, t, tile * SUBS, SUBS, cols, integrations)
                for t in range(integrations)
            ]
            while len(parts) > 1:
                parts = [a + b for a, b in zip(parts[0::2], parts[1::2])]
            summed.append(parts[0] * gain_ref[tile * SUBS : (tile + 1) * SUBS, :])
    side, room = pack_count(margin)
    for at in range(0, len(rims), side):
        packed = rims[at]
        for place, rim in enumerate(rims[at + 1 : at + side], 1):
            packed = jnp.where(lane // room == place, pltpu.roll(rim, place * room, 1), packed)
        to = 2 * bin_tiles * SUBS + at // side * SUBS
        packed_ref[to : to + SUBS, :] = packed

    def some_bins(step, tables):
        for u in range(CHUNK):
            b = first + step * CHUNK + u
            masks = [part == b for part in bins]
            stacked = jnp.zeros((SUBS, LANES), jnp.float32)
            for quantity in range(groups + 1):
                partial = jnp.zeros((SUBS, LANES), jnp.float32)
                for tile in range(tiles):
                    value = 1.0 if quantity == groups else summed[quantity * tiles + tile]
                    partial = partial + jnp.where(masks[tile], value, 0.0)
                stacked = jnp.where(row == quantity, jnp.sum(partial, axis=0, keepdims=True), stacked)
            total = jnp.sum(stacked, axis=1, keepdims=True)
            tables = tuple(
                table + jnp.where(lane == b - q * LANES, total, 0.0) for q, table in enumerate(tables)
            )
        return tables

    start = tuple(jnp.zeros((SUBS, LANES), jnp.float32) for _ in range(bin_tiles))
    tables = lax.fori_loop(0, (last - first) // CHUNK + 1, some_bins, start)
    rim_bins = jnp.broadcast_to(bins_ref[0:1, :].astype(jnp.float32), (SUBS, LANES))
    rim_bins_row = SUBS - 2 + lax.rem(lax.axis_index("freq"), 2)
    for q, table in enumerate(tables):
        shifted = pltpu.roll(table, groups + 1, 0)
        packed_ref[(bin_tiles + q) * SUBS : (bin_tiles + q + 1) * SUBS, :] = jnp.where(
            (row > groups) & (row <= 2 * groups), shifted, 0.0
        )
        if q == 0:
            table = jnp.where(row == rim_bins_row, rim_bins, table)
        packed_ref[q * SUBS : (q + 1) * SUBS, :] = table


def turn_kernel(groups, integrations, x_ref, cut_hbm, reach_hbm, turned_ref, cuts_ref, cut_ref, reach_ref, sems):
    copies = [
        pltpu.make_async_copy(cut_hbm, cut_ref, sems.at[0]),
        pltpu.make_async_copy(reach_hbm, reach_ref, sems.at[1]),
    ]
    for copy in copies:
        copy.start()
    cols = LANES // groups
    for t in range(integrations):
        block = jnp.concatenate(
            [spectra_rows(x_ref, group, t, 0, cols, cols, integrations) for group in range(groups)], axis=0
        )
        turned_ref[t * LANES : (t + 1) * LANES, :] = block.T
    for copy in copies:
        copy.wait()
    lane = lax.broadcasted_iota(jnp.int32, (1, LANES), 1)
    section = lax.axis_index("section")
    for index in range(cut_ref.shape[1]):
        for drift in range(integrations):
            line = jnp.zeros((1, LANES), jnp.float32)
            for group in range(groups):
                group_id = section * groups + group
                cut = cut_ref[group_id, index, drift].astype(jnp.float32) * (4.0 / 256.0)
                cut = jnp.where(index + 1 <= reach_ref[group_id], cut, NEVER)
                line = jnp.where(lane // cols == group, cut, line)
            at = index * integrations + drift
            cuts_ref[at : at + 1, :] = line


def look_up(rows, bins):
    found = None
    for q, values in enumerate(rows):
        spread = jnp.broadcast_to(values, bins.shape)
        index = bins if len(rows) == 1 else jnp.clip(bins - q * LANES, 0, LANES - 1)
        value = jnp.take_along_axis(spread, index, axis=1)
        found = value if q == 0 else jnp.where(bins >= q * LANES, value, found)
    return found


def inverse_levels(groups, integrations, bin_tiles, table_ref):
    first = lax.axis_index("section") * groups
    result = [[] for _ in range(groups)]
    for q in range(bin_tiles):
        rows = [table_ref[q * SUBS + r : q * SUBS + r + 1, :] for r in range(2 * groups + 1)]
        running = sum(rows[groups + 2 :], rows[groups + 1])
        for group in range(groups):
            running = running + rows[group]
            tally = rows[groups] * ((first + group + 1) * integrations).astype(jnp.float32)
            result[group].append(tally / running)
    return result


def main_kernel(
    sizes, gain_ref, bins_ref, own_ref, turned_ref, cuts_ref, normal_ref, tail_ref, head_ref, *later_refs
):
    groups, integrations = sizes.groups, sizes.integrations
    tiles = gain_ref.shape[0] // SUBS
    inverse = inverse_levels(groups, integrations, sizes.bin_tiles, own_ref)
    factors = []
    for group in range(groups):
        for tile in range(tiles):
            part = slice(tile * SUBS, (tile + 1) * SUBS)
            factors.append(look_up(inverse[group], bins_ref[part, :]) * gain_ref[part, :])
    factor = jnp.concatenate(factors, axis=0).T
    for t in range(integrations):
        normal = turned_ref[t * LANES : (t + 1) * LANES, :] * factor - 1.0
        at = t * sizes.main_span
        normal_ref[at : at + LANES, :] = normal
        normal_ref[at + LANES : at + sizes.main_span, :] = jnp.zeros((sizes.main_span - LANES, LANES), jnp.float32)
        at = t * sizes.tail_span
        tail_ref[at : at + LANES - sizes.head, :] = normal[sizes.head :]
        tail_ref[at + LANES - sizes.head : at + sizes.tail_span, :] = pltpu.roll(
            normal[: sizes.extra], LANES - 1, 1
        )
    for index in range(sizes.strides):
        scores = tree(sizes, 1, index, normal_ref, sizes.main_span, sizes.head, cuts_ref, later_refs)
        head_ref[index * sizes.head : (index + 1) * sizes.head, :] = scores


def rim_kernel(
    sizes, next_ref, rim_bins_ref, rim_ref, half_tail_ref, head_ref, cuts_ref, tail_ref, out_ref, *later_refs
):
    groups, integrations = sizes.groups, sizes.integrations
    cols = LANES // groups
    lane = lane_iota()
    at_end = lax.axis_index("freq") == lax.axis_size("freq") - 1
    inverse = inverse_levels(groups, integrations, sizes.bin_tiles, next_ref)
    rim_bins = jnp.broadcast_to(rim_bins_ref[0:1, :], (SUBS, LANES)).astype(jnp.int32)
    side, room = pack_count(sizes.margin)
    rims = []
    for group in range(groups):
        level = look_up(inverse[group], rim_bins)
        for block in range(integrations // SUBS):
            at = group * (integrations // SUBS) + block
            rim = rim_ref[at // side * SUBS : (at // side + 1) * SUBS, :]
            if at % side:
                rim = pltpu.roll(rim, LANES - at % side * room, 1)
            rims.append(jnp.where(at_end, 0.0, rim * level - 1.0))
        rims.append(jnp.zeros((cols - integrations, LANES), jnp.float32))
    edges = jnp.concatenate(rims, axis=0).T[: sizes.extra]
    lanes = lax.broadcasted_iota(jnp.int32, (sizes.extra, LANES), 1)
    for t in range(integrations):
        start = t * sizes.tail_span
        middle, end = start + LANES - sizes.head, start + sizes.tail_span
        tail_ref[start:middle, :] = half_tail_ref[start:middle, :]
        outer = pltpu.roll(edges, cols - 1 - t, 1) if cols - 1 - t else edges
        tail_ref[middle:end, :] = jnp.where(lanes % cols == cols - 1, outer, half_tail_ref[middle:end, :])
    for index in range(sizes.strides):
        head = head_ref[index * sizes.head : (index + 1) * sizes.head, :]
        rest = tree(sizes, 1, index, tail_ref, sizes.tail_span, LANES - sizes.head, cuts_ref, later_refs)
        put_scores(sizes, out_ref, index, [head, rest])


def tree_kernel(sizes, hop, normal_ref, tail_ref, cuts_ref, out_ref, *later_refs):
    half = len(later_refs) // 2
    for index in range(sizes.strides):
        head = tree(sizes, hop, index, normal_ref, sizes.main_span, sizes.head, cuts_ref, later_refs[:half])
        rest = tree(
            sizes, hop, index, tail_ref, sizes.tail_span, LANES - sizes.head, cuts_ref, later_refs[half:]
        )
        put_scores(sizes, out_ref, index, [head, rest])


def put_scores(sizes, out_ref, index, parts):
    scores = jnp.concatenate(parts, axis=0).T
    cols = LANES // sizes.groups
    for group in range(sizes.groups):
        at = (group * sizes.strides + index) * cols
        out_ref[at : at + cols, :] = scores[group * cols : (group + 1) * cols]


def tree(sizes, hop, index, normal_ref, span, length, cuts_ref, later_refs):
    integrations = sizes.integrations
    levels = integrations.bit_length() - 1
    target = lax.rem(lax.axis_index("section") + hop, lax.axis_size("section"))
    stride = target * sizes.strides + index + 1

    def values(level, block, at):
        if level == 0:
            return [normal_ref[block * span + at : block * span + at + SUBS, :]]
        former = values(level - 1, 2 * block, at)
        rows = 2 ** (level - 1)
        result = []
        for half, anchor in enumerate(former):
            if level == 1:
                ref, base = normal_ref, (2 * block + 1) * span
            else:
                ref, base = later_refs[level - 2], (block * rows + half) * span
            for steps in (half, half + 1):
                result.append(anchor + ref[pl.ds(base + at + steps * stride, SUBS), :])
        return result

    for level in range(1, levels):
        reach = min(span, length + -(-(integrations - 2**level) * sizes.rates // SUBS) * SUBS)
        reach = min(reach, span - SUBS)
        for block in range(1, integrations >> level, 2):
            for at in range(0, reach, SUBS):
                for drift, value in enumerate(values(level, block, at)):
                    row = ((block // 2) * 2**level + drift) * span + at
                    later_refs[level - 1][row : row + SUBS, :] = value
    parts = []
    for at in range(0, length, SUBS):
        score = jnp.zeros((SUBS, LANES), jnp.float32)
        for drift, value in enumerate(values(levels, 0, at)):
            cut = cuts_ref[pl.ds((stride - 1) * integrations + drift, 1), :]
            score = score + jnp.maximum(value - cut, 0.0)
        parts.append(score * (0.25 / integrations))
    return jnp.concatenate(parts, axis=0)


def far(value):
    return pltpu.with_memory_space_constraint(value, pltpu.HBM)


def swap(value, partner):
    sections, freqs = lax.axis_size("section"), lax.axis_size("freq")
    route = []
    for section in range(sections):
        for freq in range(freqs):
            to_section, to_freq = partner(section, freq)
            route.append((section * freqs + freq, to_section * freqs + to_freq))
    return lax.ppermute(value, BOTH, route)


def shards(spectra, channel_gain, bandpass_bin, drift_range, hit_cutoff):
    groups, integrations, chan_dev = spectra.shape
    sections, freqs = lax.axis_size("section"), lax.axis_size("freq")
    section, freq = lax.axis_index("section"), lax.axis_index("freq")
    total_bins = 4 * freqs
    bin_tiles = -(-total_bins // LANES)
    rates = hit_cutoff.shape[1]
    strides = rates // sections
    margin = rates * (integrations - 1)
    cols = chan_dev // LANES
    sizes = Sizes(groups, integrations, bin_tiles, margin, rates, strides)
    blocks = integrations // SUBS
    assert cols % SUBS == 0 and integrations % SUBS == 0 and margin <= LANES - SUBS
    assert sections > 1 and groups * cols == LANES and integrations <= cols
    assert freqs % 2 == 0 and 2 * groups + 1 <= SUBS - 2 and rates % sections == 0
    x = spectra.reshape(groups, blocks, SUBS, cols, LANES).transpose(0, 1, 3, 2, 4)
    x = x.reshape(groups * blocks * cols * SUBS, LANES)
    gain = channel_gain.reshape(cols, LANES)
    bins = bandpass_bin.reshape(cols, LANES)
    shape = functools.partial(jax.ShapeDtypeStruct, dtype=jnp.float32)
    side, _ = pack_count(margin)
    rim_tiles = -(-groups * blocks // side)

    packed, x_near, gain_near, bins_near = pl.pallas_call(
        functools.partial(bin_kernel, groups, integrations, bin_tiles, margin),
        out_shape=(
            shape(((2 * bin_tiles + rim_tiles) * SUBS, LANES)),
            shape(x.shape),
            shape(gain.shape),
            jax.ShapeDtypeStruct(bins.shape, bins.dtype),
        ),
        in_specs=[HBM] * 3,
        out_specs=(VMEM,) * 4,
        scratch_shapes=[pltpu.SemaphoreType.DMA((2 + groups,))],
        compiler_params=PARAMS,
        name="bin_sums",
    )(far(x), far(gain), far(bins))

    turned, cuts = pl.pallas_call(
        functools.partial(turn_kernel, groups, integrations),
        out_shape=(shape((integrations * LANES, LANES)), shape((rates * integrations, LANES))),
        in_specs=[VMEM, HBM, HBM],
        out_specs=(VMEM, VMEM),
        scratch_shapes=[
            pltpu.SMEM(hit_cutoff.shape, jnp.int32),
            pltpu.SMEM(drift_range.shape, jnp.int32),
            pltpu.SemaphoreType.DMA((2,)),
        ],
        compiler_params=PARAMS,
        cost_estimate=pl.CostEstimate(flops=10**7, bytes_accessed=0, transcendentals=0),
        name="turn",
    )(x_near, far(hit_cutoff), far(drift_range))

    mate = lambda s, f: (s, f ^ 1)

    def across(s, f):
        other = f + 1 if f % 2 else f - 1
        if 0 <= other < freqs:
            return (s, other)
        return (s ^ 1, f) if sections % 2 == 0 else (s, f)

    rows = bin_tiles * SUBS
    from_mate = swap(packed, mate)
    pairs = packed[: 2 * rows] + from_mate[: 2 * rows]
    pair, shifted_pair = pairs[:rows], pairs[rows:]
    to_across = jnp.concatenate([pair, packed[2 * rows :]], axis=0)
    to_across, shifted_pair = lax.optimization_barrier((to_across, shifted_pair))
    from_across = swap(to_across, across)
    has_across = jnp.logical_and(freq != 0, freq != freqs - 1)
    own = pair + jnp.where(has_across, from_across[:rows], 0.0)
    if sections == 2:

        def across_other(s, f):
            return (1 - s, across(s, f)[1])

        beside = swap(shifted_pair, lambda s, f: (1 - s, f))
        beside_across = swap(shifted_pair, across_other)
        earlier = beside + jnp.where(has_across, beside_across, 0.0)
        own = own + jnp.where(section == 1, earlier, 0.0)
    else:
        all_shifted = lax.all_gather(shifted_pair, "section")
        is_earlier = lax.broadcasted_iota(jnp.int32, (sections, 1, 1), 0) < section
        earlier = jnp.sum(jnp.where(is_earlier, all_shifted, 0.0), axis=0)
        earlier_across = swap(earlier, across)
        own = own + earlier + jnp.where(has_across, earlier_across, 0.0)
    odd = freq % 2 == 1
    following = jnp.where(odd, own, swap(own, mate))
    next_rim = jnp.where(odd, from_across[rows:], from_mate[2 * rows :])
    next_bins = jnp.where(odd, from_across[SUBS - 2 : SUBS - 1], from_mate[SUBS - 1 : SUBS])

    def work(flops):
        return pl.CostEstimate(flops=flops, bytes_accessed=0, transcendentals=0)

    def later(span):
        half = pltpu.VMEM((integrations // 2 * span, LANES), jnp.float32)
        return [half] * (integrations.bit_length() - 2)

    normal, half_tail, head = pl.pallas_call(
        functools.partial(main_kernel, sizes),
        out_shape=(
            shape((integrations * sizes.main_span, LANES)),
            shape((integrations * sizes.tail_span, LANES)),
            shape((strides * sizes.head, LANES)),
        ),
        in_specs=[VMEM] * 5,
        out_specs=(VMEM,) * 3,
        scratch_shapes=later(sizes.main_span),
        compiler_params=PARAMS,
        cost_estimate=work(10**7),
        name="main",
    )(gain_near, bins_near, own, turned, cuts)
    scores_shape = shape((groups * strides * cols, LANES))
    tail, first_scores = pl.pallas_call(
        functools.partial(rim_kernel, sizes),
        out_shape=(shape(half_tail.shape), scores_shape),
        in_specs=[VMEM] * 6,
        out_specs=(VMEM, VMEM),
        scratch_shapes=later(sizes.tail_span),
        compiler_params=PARAMS,
        name="rim",
    )(following, next_bins, next_rim, half_tail, head, cuts)

    def scores(hop):
        return pl.pallas_call(
            functools.partial(tree_kernel, sizes, hop),
            out_shape=scores_shape,
            in_specs=[VMEM] * 3,
            out_specs=VMEM,
            scratch_shapes=later(sizes.main_span) + later(sizes.tail_span),
            compiler_params=PARAMS,
            cost_estimate=work(10**7),
            name="tree",
        )(normal, tail, cuts)

    arrived = []
    for hop in range(1, sections):
        sent = first_scores if hop == 1 else scores(hop)
        arrived.append(swap(sent, lambda s, f: ((s + hop) % sections, f)))
    parts = [scores(0)] + arrived
    if sections == 2:
        low, high = (jnp.where(section == 0, parts[i], parts[1 - i]) for i in (0, 1))
        out = jnp.concatenate([low, high], axis=0)
    else:
        out = jnp.zeros((sections,) + parts[0].shape, jnp.float32)
        for hop, part in enumerate(parts):
            out = lax.dynamic_update_index_in_dim(out, part, (section + sections - hop) % sections, 0)
    return out.reshape(sections * groups, strides, chan_dev)


def solution(mesh):
    return jax.shard_map(
        shards,
        mesh=mesh,
        in_specs=(P("section", None, "freq"), P("freq"), P("freq"), P(), P()),
        out_specs=P(None, "section", "freq"),
        check_vma=False,
    )
```

```python
import dataclasses
import functools

import jax
import jax.numpy as jnp
from jax import lax
from jax.experimental import pallas as pl
from jax.experimental.pallas import tpu as pltpu
from jax.sharding import PartitionSpec as P

LANES = 128
SUBS = 8
BOTH = ("section", "freq")
CHUNK = 8
NEVER = 3e38
VMEM = pl.BlockSpec(memory_space=pltpu.VMEM)
SMEM = pl.BlockSpec(memory_space=pltpu.SMEM)
HBM = pl.BlockSpec(memory_space=pltpu.HBM)
PARAMS = pltpu.CompilerParams(vmem_limit_bytes=16 * 2**20)


@dataclasses.dataclass(frozen=True)
class Sizes:
    groups: int
    integrations: int
    bin_tiles: int
    margin: int
    rates: int
    strides: int

    @property
    def extra(self):
        return -(-self.margin // SUBS) * SUBS + SUBS

    @property
    def head(self):
        return LANES - -(-self.margin // SUBS) * SUBS

    @property
    def span(self):
        return LANES + self.extra

    @property
    def tail_span(self):
        return LANES - self.head + self.extra


def lane_iota():
    return lax.broadcasted_iota(jnp.int32, (SUBS, LANES), 1)


def row_iota():
    return lax.broadcasted_iota(jnp.int32, (SUBS, LANES), 0)


def spectra_rows(x_ref, group, t, first, rows, cols, integrations):
    block = group * (integrations // SUBS) + t // SUBS
    return x_ref[pl.ds((block * cols + first) * SUBS + t % SUBS, rows, stride=SUBS), :]


def pack_count(margin):
    room = 1 << (margin - 1).bit_length()
    return LANES // room, room


def bin_kernel(
    groups,
    integrations,
    bin_tiles,
    margin,
    x_hbm,
    gain_hbm,
    bins_hbm,
    packed_ref,
    x_ref,
    gain_ref,
    bins_ref,
    sems,
):
    cols = gain_ref.shape[0]
    tiles = cols // SUBS
    group_rows = integrations * cols
    copies = [
        pltpu.make_async_copy(bins_hbm, bins_ref, sems.at[0]),
        pltpu.make_async_copy(gain_hbm, gain_ref, sems.at[1]),
    ]
    for group in range(groups):
        part = pl.ds(group * group_rows, group_rows)
        copies.append(pltpu.make_async_copy(x_hbm.at[part], x_ref.at[part], sems.at[2 + group]))
    for copy in copies:
        copy.start()
    lane, row = lane_iota(), row_iota()
    copies[0].wait()
    bins = [bins_ref[tile * SUBS : (tile + 1) * SUBS, :] for tile in range(tiles)]
    first, last = jnp.min(bins[0]), jnp.max(bins[-1])
    copies[1].wait()
    summed, rims = [], []
    for group in range(groups):
        copies[2 + group].wait()
        for block in range(integrations // SUBS):
            at = (group * (integrations // SUBS) + block) * cols * SUBS
            rims.append(x_ref[at : at + SUBS, :] * gain_ref[0:1, :])
        for tile in range(tiles):
            parts = [
                spectra_rows(x_ref, group, t, tile * SUBS, SUBS, cols, integrations)
                for t in range(integrations)
            ]
            while len(parts) > 1:
                parts = [a + b for a, b in zip(parts[0::2], parts[1::2])]
            summed.append(parts[0] * gain_ref[tile * SUBS : (tile + 1) * SUBS, :])
    side, room = pack_count(margin)
    for at in range(0, len(rims), side):
        packed = rims[at]
        for place, rim in enumerate(rims[at + 1 : at + side], 1):
            packed = jnp.where(lane // room == place, pltpu.roll(rim, place * room, 1), packed)
        to = 2 * bin_tiles * SUBS + at // side * SUBS
        packed_ref[to : to + SUBS, :] = packed

    def some_bins(step, tables):
        for u in range(CHUNK):
            b = first + step * CHUNK + u
            masks = [part == b for part in bins]
            stacked = jnp.zeros((SUBS, LANES), jnp.float32)
            for quantity in range(groups + 1):
                partial = jnp.zeros((SUBS, LANES), jnp.float32)
                for tile in range(tiles):
                    value = 1.0 if quantity == groups else summed[quantity * tiles + tile]
                    partial = partial + jnp.where(masks[tile], value, 0.0)
                stacked = jnp.where(row == quantity, jnp.sum(partial, axis=0, keepdims=True), stacked)
            total = jnp.sum(stacked, axis=1, keepdims=True)
            tables = tuple(
                table + jnp.where(lane == b - q * LANES, total, 0.0) for q, table in enumerate(tables)
            )
        return tables

    start = tuple(jnp.zeros((SUBS, LANES), jnp.float32) for _ in range(bin_tiles))
    tables = lax.fori_loop(0, (last - first) // CHUNK + 1, some_bins, start)
    rim_bins = jnp.broadcast_to(bins_ref[0:1, :].astype(jnp.float32), (SUBS, LANES))
    rim_bins_row = SUBS - 2 + lax.rem(lax.axis_index("freq"), 2)
    for q, table in enumerate(tables):
        shifted = pltpu.roll(table, groups + 1, 0)
        packed_ref[(bin_tiles + q) * SUBS : (bin_tiles + q + 1) * SUBS, :] = jnp.where(
            (row > groups) & (row <= 2 * groups), shifted, 0.0
        )
        if q == 0:
            table = jnp.where(row == rim_bins_row, rim_bins, table)
        packed_ref[q * SUBS : (q + 1) * SUBS, :] = table


def turn_kernel(groups, integrations, x_ref, cut_hbm, reach_hbm, turned_ref, cuts_ref, cut_ref, reach_ref, sems):
    copies = [
        pltpu.make_async_copy(cut_hbm, cut_ref, sems.at[0]),
        pltpu.make_async_copy(reach_hbm, reach_ref, sems.at[1]),
    ]
    for copy in copies:
        copy.start()
    cols = LANES // groups
    for t in range(integrations):
        block = jnp.concatenate(
            [spectra_rows(x_ref, group, t, 0, cols, cols, integrations) for group in range(groups)], axis=0
        )
        turned_ref[t * LANES : (t + 1) * LANES, :] = block.T
    for copy in copies:
        copy.wait()
    lane = lax.broadcasted_iota(jnp.int32, (1, LANES), 1)
    section = lax.axis_index("section")
    for index in range(cut_ref.shape[1]):
        for drift in range(integrations):
            line = jnp.zeros((1, LANES), jnp.float32)
            for group in range(groups):
                group_id = section * groups + group
                cut = cut_ref[group_id, index, drift].astype(jnp.float32) * (4.0 / 256.0)
                cut = jnp.where(index + 1 <= reach_ref[group_id], cut, NEVER)
                line = jnp.where(lane // cols == group, cut, line)
            at = index * integrations + drift
            cuts_ref[at : at + 1, :] = line


def look_up(rows, bins):
    found = None
    for q, values in enumerate(rows):
        spread = jnp.broadcast_to(values, bins.shape)
        index = bins if len(rows) == 1 else jnp.clip(bins - q * LANES, 0, LANES - 1)
        value = jnp.take_along_axis(spread, index, axis=1)
        found = value if q == 0 else jnp.where(bins >= q * LANES, value, found)
    return found


def inverse_levels(groups, integrations, bin_tiles, table_ref):
    first = lax.axis_index("section") * groups
    result = [[] for _ in range(groups)]
    for q in range(bin_tiles):
        rows = [table_ref[q * SUBS + r : q * SUBS + r + 1, :] for r in range(2 * groups + 1)]
        running = sum(rows[groups + 2 :], rows[groups + 1])
        for group in range(groups):
            running = running + rows[group]
            tally = rows[groups] * ((first + group + 1) * integrations).astype(jnp.float32)
            result[group].append(tally / running)
    return result


def main_kernel(sizes, gain_ref, bins_ref, own_ref, turned_ref, cuts_ref, normal_ref, out_ref, *later_refs):
    groups, integrations = sizes.groups, sizes.integrations
    tiles = gain_ref.shape[0] // SUBS
    inverse = inverse_levels(groups, integrations, sizes.bin_tiles, own_ref)
    factors = []
    for group in range(groups):
        for tile in range(tiles):
            part = slice(tile * SUBS, (tile + 1) * SUBS)
            factors.append(look_up(inverse[group], bins_ref[part, :]) * gain_ref[part, :])
    factor = jnp.concatenate(factors, axis=0).T
    for t in range(integrations):
        normal = turned_ref[t * LANES : (t + 1) * LANES, :] * factor - 1.0
        at = t * sizes.span
        normal_ref[at : at + LANES, :] = normal
        normal_ref[at + LANES : at + sizes.span, :] = pltpu.roll(normal[: sizes.extra], LANES - 1, 1)
    for index in range(sizes.strides):
        scores = tree(sizes, 1, index, normal_ref, sizes.span, 0, LANES, cuts_ref, later_refs)
        put_scores(sizes, out_ref, index, scores.T)


def rim_kernel(sizes, hop, next_ref, rim_bins_ref, rim_ref, normal_ref, cuts_ref, tail_ref, out_ref, *later_refs):
    groups, integrations = sizes.groups, sizes.integrations
    cols = LANES // groups
    lane = lane_iota()
    at_end = lax.axis_index("freq") == lax.axis_size("freq") - 1
    inverse = inverse_levels(groups, integrations, sizes.bin_tiles, next_ref)
    rim_bins = jnp.broadcast_to(rim_bins_ref[0:1, :], (SUBS, LANES)).astype(jnp.int32)
    side, room = pack_count(sizes.margin)
    rims = []
    for group in range(groups):
        level = look_up(inverse[group], rim_bins)
        for block in range(integrations // SUBS):
            at = group * (integrations // SUBS) + block
            rim = rim_ref[at // side * SUBS : (at // side + 1) * SUBS, :]
            if at % side:
                rim = pltpu.roll(rim, LANES - at % side * room, 1)
            rims.append(jnp.where(at_end, 0.0, rim * level - 1.0))
        rims.append(jnp.zeros((cols - integrations, LANES), jnp.float32))
    edges = jnp.concatenate(rims, axis=0).T[: sizes.extra]
    lanes = lax.broadcasted_iota(jnp.int32, (sizes.extra, LANES), 1)
    for t in range(integrations):
        start = t * sizes.tail_span
        middle, end = start + LANES - sizes.head, start + sizes.tail_span
        at = t * sizes.span + sizes.head
        tail_ref[start:middle, :] = normal_ref[at : at + LANES - sizes.head, :]
        tail_ref[middle:end, :] = pltpu.roll(edges, cols - 1 - t, 1) if cols - 1 - t else edges
    put_rim_scores(sizes, hop, tail_ref, cuts_ref, out_ref, later_refs)


def own_kernel(sizes, hop, normal_ref, cuts_ref, out_ref, *later_refs):
    for index in range(sizes.strides):
        scores = tree(sizes, hop, index, normal_ref, sizes.span, 0, LANES, cuts_ref, later_refs)
        put_scores(sizes, out_ref, index, scores.T)


def last_kernel(sizes, hop, tail_ref, cuts_ref, out_ref, *later_refs):
    put_rim_scores(sizes, hop, tail_ref, cuts_ref, out_ref, later_refs)


def put_scores(sizes, out_ref, index, scores):
    cols = LANES // sizes.groups
    for group in range(sizes.groups):
        at = (group * sizes.strides + index) * cols
        out_ref[at : at + cols, :] = scores[group * cols : (group + 1) * cols]


def put_rim_scores(sizes, hop, tail_ref, cuts_ref, out_ref, later_refs):
    cols = LANES // sizes.groups
    for index in range(sizes.strides):
        rest = tree(sizes, hop, index, tail_ref, sizes.tail_span, sizes.head, LANES, cuts_ref, later_refs)
        scores = jnp.concatenate([jnp.zeros((sizes.head, LANES), jnp.float32), rest], axis=0).T
        for group in range(sizes.groups):
            at = group * sizes.strides + index
            out_ref[at : at + 1, :] = scores[(group + 1) * cols - 1 : (group + 1) * cols]


def tree(sizes, hop, index, normal_ref, span, first, last, cuts_ref, later_refs):
    integrations, length = sizes.integrations, last - first
    levels = integrations.bit_length() - 1
    target = lax.rem(lax.axis_index("section") + hop, lax.axis_size("section"))
    stride = target * sizes.strides + index + 1

    def values(level, block, at):
        if level == 0:
            return [normal_ref[block * span + at : block * span + at + SUBS, :]]
        former = values(level - 1, 2 * block, at)
        rows = 2 ** (level - 1)
        result = []
        for half, anchor in enumerate(former):
            if level == 1:
                ref, base = normal_ref, (2 * block + 1) * span
            else:
                ref, base = later_refs[level - 2], (block * rows + half) * span
            for steps in (half, half + 1):
                result.append(anchor + ref[pl.ds(base + at + steps * stride, SUBS), :])
        return result

    for level in range(1, levels):
        reach = min(span, length + -(-(integrations - 2**level) * sizes.rates // SUBS) * SUBS)
        reach = min(reach, span - SUBS)
        for block in range(1, integrations >> level, 2):
            for at in range(0, reach, SUBS):
                for drift, value in enumerate(values(level, block, at)):
                    row = ((block // 2) * 2**level + drift) * span + at
                    later_refs[level - 1][row : row + SUBS, :] = value
    parts = []
    for at in range(0, length, SUBS):
        score = jnp.zeros((SUBS, LANES), jnp.float32)
        for drift, value in enumerate(values(levels, 0, at)):
            cut = cuts_ref[pl.ds((stride - 1) * integrations + drift, 1), :]
            score = score + jnp.maximum(value - cut, 0.0)
        parts.append(score * (0.25 / integrations))
    return jnp.concatenate(parts, axis=0)


def far(value):
    return pltpu.with_memory_space_constraint(value, pltpu.HBM)


def swap(value, partner):
    sections, freqs = lax.axis_size("section"), lax.axis_size("freq")
    route = []
    for section in range(sections):
        for freq in range(freqs):
            to_section, to_freq = partner(section, freq)
            route.append((section * freqs + freq, to_section * freqs + to_freq))
    return lax.ppermute(value, BOTH, route)


def shards(spectra, channel_gain, bandpass_bin, drift_range, hit_cutoff):
    groups, integrations, chan_dev = spectra.shape
    sections, freqs = lax.axis_size("section"), lax.axis_size("freq")
    section, freq = lax.axis_index("section"), lax.axis_index("freq")
    total_bins = 4 * freqs
    bin_tiles = -(-total_bins // LANES)
    rates = hit_cutoff.shape[1]
    strides = rates // sections
    margin = rates * (integrations - 1)
    cols = chan_dev // LANES
    sizes = Sizes(groups, integrations, bin_tiles, margin, rates, strides)
    blocks = integrations // SUBS
    assert cols % SUBS == 0 and integrations % SUBS == 0 and margin <= LANES - SUBS
    assert sections > 1 and groups * cols == LANES and integrations <= cols
    assert freqs % 2 == 0 and 2 * groups + 1 <= SUBS - 2 and rates % sections == 0
    x = spectra.reshape(groups, blocks, SUBS, cols, LANES).transpose(0, 1, 3, 2, 4)
    x = x.reshape(groups * blocks * cols * SUBS, LANES)
    gain = channel_gain.reshape(cols, LANES)
    bins = bandpass_bin.reshape(cols, LANES)
    shape = functools.partial(jax.ShapeDtypeStruct, dtype=jnp.float32)
    side, _ = pack_count(margin)
    rim_tiles = -(-groups * blocks // side)

    packed, x_near, gain_near, bins_near = pl.pallas_call(
        functools.partial(bin_kernel, groups, integrations, bin_tiles, margin),
        out_shape=(
            shape(((2 * bin_tiles + rim_tiles) * SUBS, LANES)),
            shape(x.shape),
            shape(gain.shape),
            jax.ShapeDtypeStruct(bins.shape, bins.dtype),
        ),
        in_specs=[HBM] * 3,
        out_specs=(VMEM,) * 4,
        scratch_shapes=[pltpu.SemaphoreType.DMA((2 + groups,))],
        compiler_params=PARAMS,
        name="bin_sums",
    )(far(x), far(gain), far(bins))

    turned, cuts = pl.pallas_call(
        functools.partial(turn_kernel, groups, integrations),
        out_shape=(shape((integrations * LANES, LANES)), shape((rates * integrations, LANES))),
        in_specs=[VMEM, HBM, HBM],
        out_specs=(VMEM, VMEM),
        scratch_shapes=[
            pltpu.SMEM(hit_cutoff.shape, jnp.int32),
            pltpu.SMEM(drift_range.shape, jnp.int32),
            pltpu.SemaphoreType.DMA((2,)),
        ],
        compiler_params=PARAMS,
        cost_estimate=pl.CostEstimate(flops=10**7, bytes_accessed=0, transcendentals=0),
        name="turn",
    )(x_near, far(hit_cutoff), far(drift_range))

    mate = lambda s, f: (s, f ^ 1)

    def across(s, f):
        other = f + 1 if f % 2 else f - 1
        if 0 <= other < freqs:
            return (s, other)
        return (s ^ 1, f) if sections % 2 == 0 else (s, f)

    rows = bin_tiles * SUBS
    from_mate = swap(packed, mate)
    pairs = packed[: 2 * rows] + from_mate[: 2 * rows]
    pair, shifted_pair = pairs[:rows], pairs[rows:]
    to_across = jnp.concatenate([pair, packed[2 * rows :]], axis=0)
    to_across, shifted_pair = lax.optimization_barrier((to_across, shifted_pair))
    from_across = swap(to_across, across)
    has_across = jnp.logical_and(freq != 0, freq != freqs - 1)
    own = pair + jnp.where(has_across, from_across[:rows], 0.0)
    if sections == 2:

        def across_other(s, f):
            return (1 - s, across(s, f)[1])

        beside = swap(shifted_pair, lambda s, f: (1 - s, f))
        beside_across = swap(shifted_pair, across_other)
        earlier = beside + jnp.where(has_across, beside_across, 0.0)
        own = own + jnp.where(section == 1, earlier, 0.0)
    else:
        all_shifted = lax.all_gather(shifted_pair, "section")
        is_earlier = lax.broadcasted_iota(jnp.int32, (sections, 1, 1), 0) < section
        earlier = jnp.sum(jnp.where(is_earlier, all_shifted, 0.0), axis=0)
        earlier_across = swap(earlier, across)
        own = own + earlier + jnp.where(has_across, earlier_across, 0.0)
    odd = freq % 2 == 1
    following = jnp.where(odd, own, swap(own, mate))
    next_rim = jnp.where(odd, from_across[rows:], from_mate[2 * rows :])
    next_bins = jnp.where(odd, from_across[SUBS - 2 : SUBS - 1], from_mate[SUBS - 1 : SUBS])

    def work(flops):
        return pl.CostEstimate(flops=flops, bytes_accessed=0, transcendentals=0)

    def later(span):
        half = pltpu.VMEM((integrations // 2 * span, LANES), jnp.float32)
        return [half] * (integrations.bit_length() - 2)

    scores_shape = shape((groups * strides * cols, LANES))
    rim_shape = shape((-(-groups * strides // SUBS) * SUBS, LANES))
    normal, scores = pl.pallas_call(
        functools.partial(main_kernel, sizes),
        out_shape=(shape((integrations * sizes.span, LANES)), scores_shape),
        in_specs=[VMEM] * 5,
        out_specs=(VMEM, VMEM),
        scratch_shapes=later(sizes.span),
        compiler_params=PARAMS,
        cost_estimate=work(10**7),
        name="main",
    )(gain_near, bins_near, own, turned, cuts)
    tail, rim_scores = pl.pallas_call(
        functools.partial(rim_kernel, sizes, 1),
        out_shape=(shape((integrations * sizes.tail_span, LANES)), rim_shape),
        in_specs=[VMEM] * 5,
        out_specs=(VMEM, VMEM),
        scratch_shapes=later(sizes.tail_span),
        compiler_params=PARAMS,
        cost_estimate=work(10**7),
        name="rim",
    )(following, next_bins, next_rim, normal, cuts)

    def other_scores(hop):
        mostly = pl.pallas_call(
            functools.partial(own_kernel, sizes, hop),
            out_shape=scores_shape,
            in_specs=[VMEM] * 2,
            out_specs=VMEM,
            scratch_shapes=later(sizes.span),
            compiler_params=PARAMS,
            cost_estimate=work(10**7),
            name="own",
        )(normal, cuts)
        rest = pl.pallas_call(
            functools.partial(last_kernel, sizes, hop),
            out_shape=rim_shape,
            in_specs=[VMEM] * 2,
            out_specs=VMEM,
            scratch_shapes=later(sizes.tail_span),
            compiler_params=PARAMS,
            cost_estimate=work(10**7),
            name="last",
        )(tail, cuts)
        return mostly, rest

    sees_rim = jnp.logical_and(
        lax.broadcasted_iota(jnp.int32, (1, cols, LANES), 1) == cols - 1,
        lax.broadcasted_iota(jnp.int32, (1, cols, LANES), 2) >= sizes.head,
    )

    def joined(mostly, rest):
        rest = rest[: groups * strides, None, :]
        return jnp.where(sees_rim, rest, mostly.reshape(groups * strides, cols, LANES))

    arrived = []
    for hop in range(1, sections):
        to = lambda s, f: ((s + hop) % sections, f)
        mostly, rest = (scores, rim_scores) if hop == 1 else other_scores(hop)
        arrived.append(joined(swap(mostly, to), swap(rest, to)))
    parts = [joined(*other_scores(0))] + arrived
    if sections == 2:
        low, high = (jnp.where(section == 0, parts[i], parts[1 - i]) for i in (0, 1))
        out = jnp.concatenate([low, high], axis=0)
    else:
        out = jnp.zeros((sections,) + parts[0].shape, jnp.float32)
        for hop, part in enumerate(parts):
            out = lax.dynamic_update_index_in_dim(out, part, (section + sections - hop) % sections, 0)
    return out.reshape(sections * groups, strides, chan_dev)


def solution(mesh):
    return jax.shard_map(
        shards,
        mesh=mesh,
        in_specs=(P("section", None, "freq"), P("freq"), P("freq"), P(), P()),
        out_specs=P(None, "section", "freq"),
        check_vma=False,
    )
```

```python
import dataclasses
import functools

import jax
import jax.numpy as jnp
from jax import lax
from jax.experimental import pallas as pl
from jax.experimental.pallas import tpu as pltpu
from jax.sharding import PartitionSpec as P

LANES = 128
SUBS = 8
BOTH = ("section", "freq")
CHUNK = 8
NEVER = 3e38
VMEM = pl.BlockSpec(memory_space=pltpu.VMEM)
SMEM = pl.BlockSpec(memory_space=pltpu.SMEM)
HBM = pl.BlockSpec(memory_space=pltpu.HBM)
PARAMS = pltpu.CompilerParams(vmem_limit_bytes=16 * 2**20)


@dataclasses.dataclass(frozen=True)
class Sizes:
    groups: int
    integrations: int
    bin_tiles: int
    margin: int
    rates: int
    strides: int

    @property
    def extra(self):
        return -(-self.margin // SUBS) * SUBS + SUBS

    @property
    def head(self):
        return LANES - -(-self.margin // SUBS) * SUBS

    @property
    def main_span(self):
        return LANES + SUBS

    @property
    def tail_span(self):
        return LANES - self.head + self.extra


def lane_iota():
    return lax.broadcasted_iota(jnp.int32, (SUBS, LANES), 1)


def row_iota():
    return lax.broadcasted_iota(jnp.int32, (SUBS, LANES), 0)


def spectra_rows(x_ref, group, t, first, rows, cols, integrations):
    block = group * (integrations // SUBS) + t // SUBS
    return x_ref[pl.ds((block * cols + first) * SUBS + t % SUBS, rows, stride=SUBS), :]


def pack_count(margin):
    room = 1 << (margin - 1).bit_length()
    return LANES // room, room


def bin_kernel(
    groups,
    integrations,
    bin_tiles,
    margin,
    x_hbm,
    gain_hbm,
    bins_hbm,
    packed_ref,
    x_ref,
    gain_ref,
    bins_ref,
    sems,
):
    cols = gain_ref.shape[0]
    tiles = cols // SUBS
    group_rows = integrations * cols
    copies = [
        pltpu.make_async_copy(bins_hbm, bins_ref, sems.at[0]),
        pltpu.make_async_copy(gain_hbm, gain_ref, sems.at[1]),
    ]
    for group in range(groups):
        part = pl.ds(group * group_rows, group_rows)
        copies.append(pltpu.make_async_copy(x_hbm.at[part], x_ref.at[part], sems.at[2 + group]))
    for copy in copies:
        copy.start()
    lane, row = lane_iota(), row_iota()
    copies[0].wait()
    bins = [bins_ref[tile * SUBS : (tile + 1) * SUBS, :] for tile in range(tiles)]
    first, last = jnp.min(bins[0]), jnp.max(bins[-1])
    copies[1].wait()
    summed, rims = [], []
    for group in range(groups):
        copies[2 + group].wait()
        for block in range(integrations // SUBS):
            at = (group * (integrations // SUBS) + block) * cols * SUBS
            rims.append(x_ref[at : at + SUBS, :] * gain_ref[0:1, :])
        for tile in range(tiles):
            parts = [
                spectra_rows(x_ref, group, t, tile * SUBS, SUBS, cols, integrations)
                for t in range(integrations)
            ]
            while len(parts) > 1:
                parts = [a + b for a, b in zip(parts[0::2], parts[1::2])]
            summed.append(parts[0] * gain_ref[tile * SUBS : (tile + 1) * SUBS, :])
    side, room = pack_count(margin)
    for at in range(0, len(rims), side):
        packed = rims[at]
        for place, rim in enumerate(rims[at + 1 : at + side], 1):
            packed = jnp.where(lane // room == place, pltpu.roll(rim, place * room, 1), packed)
        to = 2 * bin_tiles * SUBS + at // side * SUBS
        packed_ref[to : to + SUBS, :] = packed

    def some_bins(step, tables):
        for u in range(CHUNK):
            b = first + step * CHUNK + u
            masks = [part == b for part in bins]
            stacked = jnp.zeros((SUBS, LANES), jnp.float32)
            for quantity in range(groups + 1):
                partial = jnp.zeros((SUBS, LANES), jnp.float32)
                for tile in range(tiles):
                    value = 1.0 if quantity == groups else summed[quantity * tiles + tile]
                    partial = partial + jnp.where(masks[tile], value, 0.0)
                stacked = jnp.where(row == quantity, jnp.sum(partial, axis=0, keepdims=True), stacked)
            total = jnp.sum(stacked, axis=1, keepdims=True)
            tables = tuple(
                table + jnp.where(lane == b - q * LANES, total, 0.0) for q, table in enumerate(tables)
            )
        return tables

    start = tuple(jnp.zeros((SUBS, LANES), jnp.float32) for _ in range(bin_tiles))
    tables = lax.fori_loop(0, (last - first) // CHUNK + 1, some_bins, start)
    rim_bins = jnp.broadcast_to(bins_ref[0:1, :].astype(jnp.float32), (SUBS, LANES))
    rim_bins_row = SUBS - 2 + lax.rem(lax.axis_index("freq"), 2)
    for q, table in enumerate(tables):
        shifted = pltpu.roll(table, groups + 1, 0)
        packed_ref[(bin_tiles + q) * SUBS : (bin_tiles + q + 1) * SUBS, :] = jnp.where(
            (row > groups) & (row <= 2 * groups), shifted, 0.0
        )
        if q == 0:
            table = jnp.where(row == rim_bins_row, rim_bins, table)
        packed_ref[q * SUBS : (q + 1) * SUBS, :] = table


def turn_kernel(groups, integrations, x_ref, cut_hbm, reach_hbm, turned_ref, cuts_ref, cut_ref, reach_ref, sems):
    copies = [
        pltpu.make_async_copy(cut_hbm, cut_ref, sems.at[0]),
        pltpu.make_async_copy(reach_hbm, reach_ref, sems.at[1]),
    ]
    for copy in copies:
        copy.start()
    cols = LANES // groups
    for t in range(integrations):
        block = jnp.concatenate(
            [spectra_rows(x_ref, group, t, 0, cols, cols, integrations) for group in range(groups)], axis=0
        )
        turned_ref[t * LANES : (t + 1) * LANES, :] = block.T
    for copy in copies:
        copy.wait()
    lane = lax.broadcasted_iota(jnp.int32, (1, LANES), 1)
    section = lax.axis_index("section")
    for index in range(cut_ref.shape[1]):
        for drift in range(integrations):
            line = jnp.zeros((1, LANES), jnp.float32)
            for group in range(groups):
                group_id = section * groups + group
                cut = cut_ref[group_id, index, drift].astype(jnp.float32) * (4.0 / 256.0)
                cut = jnp.where(index + 1 <= reach_ref[group_id], cut, NEVER)
                line = jnp.where(lane // cols == group, cut, line)
            at = index * integrations + drift
            cuts_ref[at : at + 1, :] = line


def look_up(rows, bins):
    found = None
    for q, values in enumerate(rows):
        spread = jnp.broadcast_to(values, bins.shape)
        index = bins if len(rows) == 1 else jnp.clip(bins - q * LANES, 0, LANES - 1)
        value = jnp.take_along_axis(spread, index, axis=1)
        found = value if q == 0 else jnp.where(bins >= q * LANES, value, found)
    return found


def inverse_levels(groups, integrations, bin_tiles, table_ref):
    first = lax.axis_index("section") * groups
    result = [[] for _ in range(groups)]
    for q in range(bin_tiles):
        rows = [table_ref[q * SUBS + r : q * SUBS + r + 1, :] for r in range(2 * groups + 1)]
        running = sum(rows[groups + 2 :], rows[groups + 1])
        for group in range(groups):
            running = running + rows[group]
            tally = rows[groups] * ((first + group + 1) * integrations).astype(jnp.float32)
            result[group].append(tally / running)
    return result


def main_kernel(
    sizes, gain_ref, bins_ref, own_ref, turned_ref, cuts_ref, normal_ref, tail_ref, head_ref, *later_refs
):
    groups, integrations = sizes.groups, sizes.integrations
    tiles = gain_ref.shape[0] // SUBS
    inverse = inverse_levels(groups, integrations, sizes.bin_tiles, own_ref)
    factors = []
    for group in range(groups):
        for tile in range(tiles):
            part = slice(tile * SUBS, (tile + 1) * SUBS)
            factors.append(look_up(inverse[group], bins_ref[part, :]) * gain_ref[part, :])
    factor = jnp.concatenate(factors, axis=0).T
    for t in range(integrations):
        normal = turned_ref[t * LANES : (t + 1) * LANES, :] * factor - 1.0
        at = t * sizes.main_span
        normal_ref[at : at + LANES, :] = normal
        normal_ref[at + LANES : at + sizes.main_span, :] = jnp.zeros((sizes.main_span - LANES, LANES), jnp.float32)
        at = t * sizes.tail_span
        tail_ref[at : at + LANES - sizes.head, :] = normal[sizes.head :]
        tail_ref[at + LANES - sizes.head : at + sizes.tail_span, :] = pltpu.roll(
            normal[: sizes.extra], LANES - 1, 1
        )
    for index in range(sizes.strides):
        scores = tree(sizes, 1, index, normal_ref, sizes.main_span, sizes.head, cuts_ref, later_refs)
        head_ref[index * sizes.head : (index + 1) * sizes.head, :] = scores


def rim_kernel(
    sizes, next_ref, rim_bins_ref, rim_ref, half_tail_ref, head_ref, cuts_ref, tail_ref, out_ref, *later_refs
):
    groups, integrations = sizes.groups, sizes.integrations
    cols = LANES // groups
    lane = lane_iota()
    at_end = lax.axis_index("freq") == lax.axis_size("freq") - 1
    inverse = inverse_levels(groups, integrations, sizes.bin_tiles, next_ref)
    rim_bins = jnp.broadcast_to(rim_bins_ref[0:1, :], (SUBS, LANES)).astype(jnp.int32)
    side, room = pack_count(sizes.margin)
    rims = []
    for group in range(groups):
        level = look_up(inverse[group], rim_bins)
        for block in range(integrations // SUBS):
            at = group * (integrations // SUBS) + block
            rim = rim_ref[at // side * SUBS : (at // side + 1) * SUBS, :]
            if at % side:
                rim = pltpu.roll(rim, LANES - at % side * room, 1)
            rims.append(jnp.where(at_end, 0.0, rim * level - 1.0))
        rims.append(jnp.zeros((cols - integrations, LANES), jnp.float32))
    edges = jnp.concatenate(rims, axis=0).T[: sizes.extra]
    lanes = lax.broadcasted_iota(jnp.int32, (sizes.extra, LANES), 1)
    for t in range(integrations):
        start = t * sizes.tail_span
        middle, end = start + LANES - sizes.head, start + sizes.tail_span
        tail_ref[start:middle, :] = half_tail_ref[start:middle, :]
        outer = pltpu.roll(edges, cols - 1 - t, 1) if cols - 1 - t else edges
        tail_ref[middle:end, :] = jnp.where(lanes % cols == cols - 1, outer, half_tail_ref[middle:end, :])
    for index in range(sizes.strides):
        head = head_ref[index * sizes.head : (index + 1) * sizes.head, :]
        rest = tree(sizes, 1, index, tail_ref, sizes.tail_span, LANES - sizes.head, cuts_ref, later_refs)
        put_scores(sizes, out_ref, index, [head, rest])


def tree_kernel(sizes, hop, normal_ref, tail_ref, cuts_ref, out_ref, *later_refs):
    half = len(later_refs) // 2
    for index in range(sizes.strides):
        head = tree(sizes, hop, index, normal_ref, sizes.main_span, sizes.head, cuts_ref, later_refs[:half])
        rest = tree(
            sizes, hop, index, tail_ref, sizes.tail_span, LANES - sizes.head, cuts_ref, later_refs[half:]
        )
        put_scores(sizes, out_ref, index, [head, rest])


def put_scores(sizes, out_ref, index, parts):
    scores = jnp.concatenate(parts, axis=0).T
    cols = LANES // sizes.groups
    for group in range(sizes.groups):
        at = (group * sizes.strides + index) * cols
        out_ref[at : at + cols, :] = scores[group * cols : (group + 1) * cols]


def tree(sizes, hop, index, normal_ref, span, length, cuts_ref, later_refs):
    integrations = sizes.integrations
    levels = integrations.bit_length() - 1
    target = lax.rem(lax.axis_index("section") + hop, lax.axis_size("section"))
    stride = target * sizes.strides + index + 1

    def values(level, block, at):
        if level == 0:
            return [normal_ref[block * span + at : block * span + at + SUBS, :]]
        former = values(level - 1, 2 * block, at)
        rows = 2 ** (level - 1)
        result = []
        for half, anchor in enumerate(former):
            if level == 1:
                ref, base = normal_ref, (2 * block + 1) * span
            else:
                ref, base = later_refs[level - 2], (block * rows + half) * span
            for steps in (half, half + 1):
                result.append(anchor + ref[pl.ds(base + at + steps * stride, SUBS), :])
        return result

    for level in range(1, levels):
        reach = min(span, length + -(-(integrations - 2**level) * sizes.rates // SUBS) * SUBS)
        reach = min(reach, span - SUBS)
        for block in range(1, integrations >> level, 2):
            for at in range(0, reach, SUBS):
                for drift, value in enumerate(values(level, block, at)):
                    row = ((block // 2) * 2**level + drift) * span + at
                    later_refs[level - 1][row : row + SUBS, :] = value
    parts = []
    for at in range(0, length, SUBS):
        score = jnp.zeros((SUBS, LANES), jnp.float32)
        for drift, value in enumerate(values(levels, 0, at)):
            cut = cuts_ref[pl.ds((stride - 1) * integrations + drift, 1), :]
            score = score + jnp.maximum(value - cut, 0.0)
        parts.append(score * (0.25 / integrations))
    return jnp.concatenate(parts, axis=0)


def far(value):
    return pltpu.with_memory_space_constraint(value, pltpu.HBM)


def swap(value, partner):
    sections, freqs = lax.axis_size("section"), lax.axis_size("freq")
    route = []
    for section in range(sections):
        for freq in range(freqs):
            to_section, to_freq = partner(section, freq)
            route.append((section * freqs + freq, to_section * freqs + to_freq))
    return lax.ppermute(value, BOTH, route)


def shards(spectra, channel_gain, bandpass_bin, drift_range, hit_cutoff):
    groups, integrations, chan_dev = spectra.shape
    sections, freqs = lax.axis_size("section"), lax.axis_size("freq")
    section, freq = lax.axis_index("section"), lax.axis_index("freq")
    total_bins = 4 * freqs
    bin_tiles = -(-total_bins // LANES)
    rates = hit_cutoff.shape[1]
    strides = rates // sections
    margin = rates * (integrations - 1)
    cols = chan_dev // LANES
    sizes = Sizes(groups, integrations, bin_tiles, margin, rates, strides)
    blocks = integrations // SUBS
    assert cols % SUBS == 0 and integrations % SUBS == 0 and margin <= LANES - SUBS
    assert sections > 1 and groups * cols == LANES and integrations <= cols
    assert freqs % 2 == 0 and 2 * groups + 1 <= SUBS - 2 and rates % sections == 0
    x = spectra.reshape(groups, blocks, SUBS, cols, LANES).transpose(0, 1, 3, 2, 4)
    x = x.reshape(groups * blocks * cols * SUBS, LANES)
    gain = channel_gain.reshape(cols, LANES)
    bins = bandpass_bin.reshape(cols, LANES)
    shape = functools.partial(jax.ShapeDtypeStruct, dtype=jnp.float32)
    side, _ = pack_count(margin)
    rim_tiles = -(-groups * blocks // side)

    packed, x_near, gain_near, bins_near = pl.pallas_call(
        functools.partial(bin_kernel, groups, integrations, bin_tiles, margin),
        out_shape=(
            shape(((2 * bin_tiles + rim_tiles) * SUBS, LANES)),
            shape(x.shape),
            shape(gain.shape),
            jax.ShapeDtypeStruct(bins.shape, bins.dtype),
        ),
        in_specs=[HBM] * 3,
        out_specs=(VMEM,) * 4,
        scratch_shapes=[pltpu.SemaphoreType.DMA((2 + groups,))],
        compiler_params=PARAMS,
        name="bin_sums",
    )(far(x), far(gain), far(bins))

    turned, cuts = pl.pallas_call(
        functools.partial(turn_kernel, groups, integrations),
        out_shape=(shape((integrations * LANES, LANES)), shape((rates * integrations, LANES))),
        in_specs=[VMEM, HBM, HBM],
        out_specs=(VMEM, VMEM),
        scratch_shapes=[
            pltpu.SMEM(hit_cutoff.shape, jnp.int32),
            pltpu.SMEM(drift_range.shape, jnp.int32),
            pltpu.SemaphoreType.DMA((2,)),
        ],
        compiler_params=PARAMS,
        cost_estimate=pl.CostEstimate(flops=10**7, bytes_accessed=0, transcendentals=0),
        name="turn",
    )(x_near, far(hit_cutoff), far(drift_range))

    mate = lambda s, f: (s, f ^ 1)

    def across(s, f):
        other = f + 1 if f % 2 else f - 1
        if 0 <= other < freqs:
            return (s, other)
        return (s ^ 1, f) if sections % 2 == 0 else (s, f)

    rows = bin_tiles * SUBS
    from_mate = swap(packed, mate)
    pairs = packed[: 2 * rows] + from_mate[: 2 * rows]
    pair, shifted_pair = pairs[:rows], pairs[rows:]
    to_across = jnp.concatenate([pair, packed[2 * rows :]], axis=0)
    to_across, shifted_pair = lax.optimization_barrier((to_across, shifted_pair))
    from_across = swap(to_across, across)
    has_across = jnp.logical_and(freq != 0, freq != freqs - 1)
    own = pair + jnp.where(has_across, from_across[:rows], 0.0)
    if sections == 2:

        def across_other(s, f):
            return (1, across(s, f)[1]) if s == 0 else (0, f)

        beside = swap(shifted_pair, lambda s, f: (1 - s, f))
        beside_across = swap(shifted_pair, across_other)
        earlier = beside + jnp.where(has_across, beside_across, 0.0)
        own = own + jnp.where(section == 1, earlier, 0.0)
    else:
        all_shifted = lax.all_gather(shifted_pair, "section")
        is_earlier = lax.broadcasted_iota(jnp.int32, (sections, 1, 1), 0) < section
        earlier = jnp.sum(jnp.where(is_earlier, all_shifted, 0.0), axis=0)
        earlier_across = swap(earlier, across)
        own = own + earlier + jnp.where(has_across, earlier_across, 0.0)
    odd = freq % 2 == 1
    following = jnp.where(odd, own, swap(own, mate))
    next_rim = jnp.where(odd, from_across[rows:], from_mate[2 * rows :])
    next_bins = jnp.where(odd, from_across[SUBS - 2 : SUBS - 1], from_mate[SUBS - 1 : SUBS])

    def work(flops):
        return pl.CostEstimate(flops=flops, bytes_accessed=0, transcendentals=0)

    def later(span):
        half = pltpu.VMEM((integrations // 2 * span, LANES), jnp.float32)
        return [half] * (integrations.bit_length() - 2)

    normal, half_tail, head = pl.pallas_call(
        functools.partial(main_kernel, sizes),
        out_shape=(
            shape((integrations * sizes.main_span, LANES)),
            shape((integrations * sizes.tail_span, LANES)),
            shape((strides * sizes.head, LANES)),
        ),
        in_specs=[VMEM] * 5,
        out_specs=(VMEM,) * 3,
        scratch_shapes=later(sizes.main_span),
        compiler_params=PARAMS,
        cost_estimate=work(10**7),
        name="main",
    )(gain_near, bins_near, own, turned, cuts)
    scores_shape = shape((groups * strides * cols, LANES))
    tail, first_scores = pl.pallas_call(
        functools.partial(rim_kernel, sizes),
        out_shape=(shape(half_tail.shape), scores_shape),
        in_specs=[VMEM] * 6,
        out_specs=(VMEM, VMEM),
        scratch_shapes=later(sizes.tail_span),
        compiler_params=PARAMS,
        name="rim",
    )(following, next_bins, next_rim, half_tail, head, cuts)

    def scores(hop):
        return pl.pallas_call(
            functools.partial(tree_kernel, sizes, hop),
            out_shape=scores_shape,
            in_specs=[VMEM] * 3,
            out_specs=VMEM,
            scratch_shapes=later(sizes.main_span) + later(sizes.tail_span),
            compiler_params=PARAMS,
            cost_estimate=work(10**7),
            name="tree",
        )(normal, tail, cuts)

    arrived = []
    for hop in range(1, sections):
        sent = first_scores if hop == 1 else scores(hop)
        arrived.append(swap(sent, lambda s, f: ((s + hop) % sections, f)))
    parts = [scores(0)] + arrived
    if sections == 2:
        low, high = (jnp.where(section == 0, parts[i], parts[1 - i]) for i in (0, 1))
        out = jnp.concatenate([low, high], axis=0)
    else:
        out = jnp.zeros((sections,) + parts[0].shape, jnp.float32)
        for hop, part in enumerate(parts):
            out = lax.dynamic_update_index_in_dim(out, part, (section + sections - hop) % sections, 0)
    return out.reshape(sections * groups, strides, chan_dev)


def solution(mesh):
    return jax.shard_map(
        shards,
        mesh=mesh,
        in_specs=(P("section", None, "freq"), P("freq"), P("freq"), P(), P()),
        out_specs=P(None, "section", "freq"),
        check_vma=False,
    )
```

```python
import dataclasses
import functools

import jax
import jax.numpy as jnp
from jax import lax
from jax.experimental import pallas as pl
from jax.experimental.pallas import tpu as pltpu
from jax.sharding import PartitionSpec as P


LANES = 128
SUBS = 8
BOTH = ("section", "freq")
CHUNK = 8
NEVER = 3e38
VMEM = pl.BlockSpec(memory_space=pltpu.VMEM)
SMEM = pl.BlockSpec(memory_space=pltpu.SMEM)
HBM = pl.BlockSpec(memory_space=pltpu.HBM)
PARAMS = pltpu.CompilerParams(vmem_limit_bytes=16 * 2**20)


@dataclasses.dataclass(frozen=True)
class Sizes:
    groups: int
    integrations: int
    bin_tiles: int
    margin: int
    rates: int
    strides: int

    @property
    def extra(self):
        return -(-self.margin // SUBS) * SUBS + SUBS

    @property
    def head(self):
        return LANES - -(-self.margin // SUBS) * SUBS

    @property
    def main_span(self):
        return LANES + SUBS

    @property
    def tail_span(self):
        return LANES - self.head + self.extra


def lane_iota():
    return lax.broadcasted_iota(jnp.int32, (SUBS, LANES), 1)


def row_iota():
    return lax.broadcasted_iota(jnp.int32, (SUBS, LANES), 0)


def spectra_rows(x_ref, group, t, first, rows, cols, integrations):
    block = group * (integrations // SUBS) + t // SUBS
    return x_ref[pl.ds((block * cols + first) * SUBS + t % SUBS, rows, stride=SUBS), :]


def pack_count(margin):
    room = 1 << (margin - 1).bit_length()
    return LANES // room, room


def bin_kernel(
    groups,
    integrations,
    bin_tiles,
    margin,
    x_hbm,
    gain_hbm,
    bins_hbm,
    packed_ref,
    x_ref,
    gain_ref,
    bins_ref,
    sems,
):
    cols = gain_ref.shape[0]
    tiles = cols // SUBS
    group_rows = integrations * cols
    copies = [
        pltpu.make_async_copy(bins_hbm, bins_ref, sems.at[0]),
        pltpu.make_async_copy(gain_hbm, gain_ref, sems.at[1]),
    ]
    for group in range(groups):
        part = pl.ds(group * group_rows, group_rows)
        copies.append(pltpu.make_async_copy(x_hbm.at[part], x_ref.at[part], sems.at[2 + group]))
    for copy in copies:
        copy.start()
    lane, row = lane_iota(), row_iota()
    copies[0].wait()
    bins = [bins_ref[tile * SUBS : (tile + 1) * SUBS, :] for tile in range(tiles)]
    first, last = jnp.min(bins[0]), jnp.max(bins[-1])
    copies[1].wait()
    summed, rims = [], []
    for group in range(groups):
        copies[2 + group].wait()
        for block in range(integrations // SUBS):
            at = (group * (integrations // SUBS) + block) * cols * SUBS
            rims.append(x_ref[at : at + SUBS, :] * gain_ref[0:1, :])
        for tile in range(tiles):
            parts = [
                spectra_rows(x_ref, group, t, tile * SUBS, SUBS, cols, integrations)
                for t in range(integrations)
            ]
            while len(parts) > 1:
                parts = [a + b for a, b in zip(parts[0::2], parts[1::2])]
            summed.append(parts[0] * gain_ref[tile * SUBS : (tile + 1) * SUBS, :])
    side, room = pack_count(margin)
    for at in range(0, len(rims), side):
        packed = rims[at]
        for place, rim in enumerate(rims[at + 1 : at + side], 1):
            packed = jnp.where(lane // room == place, pltpu.roll(rim, place * room, 1), packed)
        to = 2 * bin_tiles * SUBS + at // side * SUBS
        packed_ref[to : to + SUBS, :] = packed

    def some_bins(step, tables):
        for u in range(CHUNK):
            b = first + step * CHUNK + u
            masks = [part == b for part in bins]
            stacked = jnp.zeros((SUBS, LANES), jnp.float32)
            for quantity in range(groups + 1):
                partial = jnp.zeros((SUBS, LANES), jnp.float32)
                for tile in range(tiles):
                    value = 1.0 if quantity == groups else summed[quantity * tiles + tile]
                    partial = partial + jnp.where(masks[tile], value, 0.0)
                stacked = jnp.where(row == quantity, jnp.sum(partial, axis=0, keepdims=True), stacked)
            total = jnp.sum(stacked, axis=1, keepdims=True)
            tables = tuple(
                table + jnp.where(lane == b - q * LANES, total, 0.0) for q, table in enumerate(tables)
            )
        return tables

    start = tuple(jnp.zeros((SUBS, LANES), jnp.float32) for _ in range(bin_tiles))
    tables = lax.fori_loop(0, (last - first) // CHUNK + 1, some_bins, start)
    rim_bins = jnp.broadcast_to(bins_ref[0:1, :].astype(jnp.float32), (SUBS, LANES))
    rim_bins_row = SUBS - 2 + lax.rem(lax.axis_index("freq"), 2)
    for q, table in enumerate(tables):
        shifted = pltpu.roll(table, groups + 1, 0)
        packed_ref[(bin_tiles + q) * SUBS : (bin_tiles + q + 1) * SUBS, :] = jnp.where(
            (row > groups) & (row <= 2 * groups), shifted, 0.0
        )
        if q == 0:
            table = jnp.where(row == rim_bins_row, rim_bins, table)
        packed_ref[q * SUBS : (q + 1) * SUBS, :] = table


def turn_kernel(groups, integrations, x_ref, cut_hbm, reach_hbm, turned_ref, cuts_ref, cut_ref, reach_ref, sems):
    copies = [
        pltpu.make_async_copy(cut_hbm, cut_ref, sems.at[0]),
        pltpu.make_async_copy(reach_hbm, reach_ref, sems.at[1]),
    ]
    for copy in copies:
        copy.start()
    cols = LANES // groups
    for t in range(integrations):
        block = jnp.concatenate(
            [spectra_rows(x_ref, group, t, 0, cols, cols, integrations) for group in range(groups)], axis=0
        )
        turned_ref[t * LANES : (t + 1) * LANES, :] = block.T
    for copy in copies:
        copy.wait()
    lane = lax.broadcasted_iota(jnp.int32, (1, LANES), 1)
    section = lax.axis_index("section")
    for index in range(cut_ref.shape[1]):
        for drift in range(integrations):
            line = jnp.zeros((1, LANES), jnp.float32)
            for group in range(groups):
                group_id = section * groups + group
                cut = cut_ref[group_id, index, drift].astype(jnp.float32) * (4.0 / 256.0)
                cut = jnp.where(index + 1 <= reach_ref[group_id], cut, NEVER)
                line = jnp.where(lane // cols == group, cut, line)
            at = index * integrations + drift
            cuts_ref[at : at + 1, :] = line


def look_up(rows, bins):
    found = None
    for q, values in enumerate(rows):
        spread = jnp.broadcast_to(values, bins.shape)
        index = bins if len(rows) == 1 else jnp.clip(bins - q * LANES, 0, LANES - 1)
        value = jnp.take_along_axis(spread, index, axis=1)
        found = value if q == 0 else jnp.where(bins >= q * LANES, value, found)
    return found


def inverse_levels(groups, integrations, bin_tiles, table_ref):
    first = lax.axis_index("section") * groups
    result = [[] for _ in range(groups)]
    for q in range(bin_tiles):
        rows = [table_ref[q * SUBS + r : q * SUBS + r + 1, :] for r in range(2 * groups + 1)]
        running = sum(rows[groups + 2 :], rows[groups + 1])
        for group in range(groups):
            running = running + rows[group]
            tally = rows[groups] * ((first + group + 1) * integrations).astype(jnp.float32)
            result[group].append(tally / running)
    return result


def main_kernel(
    sizes,
    gain_ref,
    bins_ref,
    own_ref,
    rim_bins_ref,
    rim_ref,
    turned_ref,
    cuts_ref,
    normal_ref,
    tail_ref,
    rim_index_ref,
    head_ref,
    *later_refs,
):
    groups, integrations = sizes.groups, sizes.integrations
    tiles = gain_ref.shape[0] // SUBS
    inverse = inverse_levels(groups, integrations, sizes.bin_tiles, own_ref)
    factors = []
    for group in range(groups):
        for tile in range(tiles):
            part = slice(tile * SUBS, (tile + 1) * SUBS)
            factors.append(look_up(inverse[group], bins_ref[part, :]) * gain_ref[part, :])
    factor = jnp.concatenate(factors, axis=0).T
    cols = LANES // groups
    side, room = pack_count(sizes.margin)
    rims = []
    for group in range(groups):
        for block in range(integrations // SUBS):
            at = group * (integrations // SUBS) + block
            rim = rim_ref[at // side * SUBS : (at // side + 1) * SUBS, :]
            rims.append(pltpu.roll(rim, LANES - at % side * room, 1) if at % side else rim)
        rims.append(jnp.zeros((cols - integrations, LANES), jnp.float32))
    raw = jnp.concatenate(rims, axis=0).T[: sizes.extra]
    rim_index = jnp.broadcast_to(rim_bins_ref[0:1, :], (LANES, LANES)).T
    rim_index_ref[...] = rim_index[: sizes.extra].astype(jnp.int32)
    last_col = lax.broadcasted_iota(jnp.int32, (sizes.extra, LANES), 1) % cols == cols - 1
    for t in range(integrations):
        normal = turned_ref[t * LANES : (t + 1) * LANES, :] * factor - 1.0
        at = t * sizes.main_span
        normal_ref[at : at + LANES, :] = normal
        normal_ref[at + LANES : at + sizes.main_span, :] = jnp.zeros((sizes.main_span - LANES, LANES), jnp.float32)
        at = t * sizes.tail_span
        tail_ref[at : at + LANES - sizes.head, :] = normal[sizes.head :]
        outer = pltpu.roll(raw, cols - 1 - t, 1) if cols - 1 - t else raw
        tail_ref[at + LANES - sizes.head : at + sizes.tail_span, :] = jnp.where(
            last_col, outer, pltpu.roll(normal[: sizes.extra], LANES - 1, 1)
        )
    for index in range(sizes.strides):
        scores = tree(sizes, 1, index, normal_ref, sizes.main_span, sizes.head, cuts_ref, later_refs)
        head_ref[index * sizes.head : (index + 1) * sizes.head, :] = scores


def rim_kernel(
    sizes, next_ref, rim_index_ref, half_tail_ref, head_ref, cuts_ref, tail_ref, out_ref, *later_refs
):
    groups, integrations = sizes.groups, sizes.integrations
    cols = LANES // groups
    lane = lane_iota()
    at_end = lax.axis_index("freq") == lax.axis_size("freq") - 1
    last_col = lane % cols == cols - 1
    inverse = inverse_levels(groups, integrations, sizes.bin_tiles, next_ref)
    inner = LANES - sizes.head
    for row in range(0, sizes.extra, SUBS):
        index = rim_index_ref[row : row + SUBS, :]
        level = look_up(inverse[0], index)
        for group in range(1, groups):
            level = jnp.where(lane // cols == group, look_up(inverse[group], index), level)
        for t in range(integrations):
            at = t * sizes.tail_span + inner + row
            half = half_tail_ref[at : at + SUBS, :]
            edge = jnp.where(at_end, 0.0, half * level - 1.0)
            tail_ref[at : at + SUBS, :] = jnp.where(last_col, edge, half)
    for t in range(integrations):
        at = t * sizes.tail_span
        tail_ref[at : at + inner, :] = half_tail_ref[at : at + inner, :]
    for index in range(sizes.strides):
        head = head_ref[index * sizes.head : (index + 1) * sizes.head, :]
        rest = tree(sizes, 1, index, tail_ref, sizes.tail_span, LANES - sizes.head, cuts_ref, later_refs)
        put_scores(sizes, out_ref, index, [head, rest])


def tree_kernel(sizes, hop, normal_ref, tail_ref, cuts_ref, out_ref, *later_refs):
    half = len(later_refs) // 2
    for index in range(sizes.strides):
        head = tree(sizes, hop, index, normal_ref, sizes.main_span, sizes.head, cuts_ref, later_refs[:half])
        rest = tree(
            sizes, hop, index, tail_ref, sizes.tail_span, LANES - sizes.head, cuts_ref, later_refs[half:]
        )
        put_scores(sizes, out_ref, index, [head, rest])


def own_kernel(sizes, normal_ref, tail_ref, cuts_ref, out_hbm, scores_ref, sem, *later_refs):
    tree_kernel(sizes, 0, normal_ref, tail_ref, cuts_ref, scores_ref, *later_refs)
    rows = scores_ref.shape[0]
    at = pl.multiple_of(lax.axis_index("section") * rows, SUBS)
    copy = pltpu.make_async_copy(scores_ref, out_hbm.at[pl.ds(at, rows)], sem)
    copy.start()
    copy.wait()


def place_kernel(hop, scores_ref, _, out_hbm, sem):
    rows, sections = scores_ref.shape[0], lax.axis_size("section")
    at = pl.multiple_of(lax.rem(lax.axis_index("section") + sections - hop, sections) * rows, SUBS)
    copy = pltpu.make_async_copy(scores_ref, out_hbm.at[pl.ds(at, rows)], sem)
    copy.start()
    copy.wait()


def put_scores(sizes, out_ref, index, parts):
    scores = jnp.concatenate(parts, axis=0).T
    cols = LANES // sizes.groups
    for group in range(sizes.groups):
        at = (group * sizes.strides + index) * cols
        out_ref[at : at + cols, :] = scores[group * cols : (group + 1) * cols]


def tree(sizes, hop, index, normal_ref, span, length, cuts_ref, later_refs):
    integrations = sizes.integrations
    levels = integrations.bit_length() - 1
    target = lax.rem(lax.axis_index("section") + hop, lax.axis_size("section"))
    stride = target * sizes.strides + index + 1

    def values(level, block, at):
        if level == 0:
            return [normal_ref[block * span + at : block * span + at + SUBS, :]]
        former = values(level - 1, 2 * block, at)
        rows = 2 ** (level - 1)
        result = []
        for half, anchor in enumerate(former):
            if level == 1:
                ref, base = normal_ref, (2 * block + 1) * span
            else:
                ref, base = later_refs[level - 2], (block * rows + half) * span
            for steps in (half, half + 1):
                result.append(anchor + ref[pl.ds(base + at + steps * stride, SUBS), :])
        return result

    for level in range(1, levels):
        reach = min(span, length + -(-(integrations - 2**level) * sizes.rates // SUBS) * SUBS)
        reach = min(reach, span - SUBS)
        for block in range(1, integrations >> level, 2):
            for at in range(0, reach, SUBS):
                for drift, value in enumerate(values(level, block, at)):
                    row = ((block // 2) * 2**level + drift) * span + at
                    later_refs[level - 1][row : row + SUBS, :] = value
    parts = []
    for at in range(0, length, SUBS):
        score = jnp.zeros((SUBS, LANES), jnp.float32)
        for drift, value in enumerate(values(levels, 0, at)):
            cut = cuts_ref[pl.ds((stride - 1) * integrations + drift, 1), :]
            score = score + jnp.maximum(value - cut, 0.0)
        parts.append(score * (0.25 / integrations))
    return jnp.concatenate(parts, axis=0)


def far(value):
    return pltpu.with_memory_space_constraint(value, pltpu.HBM)


def swap(value, partner):
    sections, freqs = lax.axis_size("section"), lax.axis_size("freq")
    route = []
    for section in range(sections):
        for freq in range(freqs):
            to_section, to_freq = partner(section, freq)
            route.append((section * freqs + freq, to_section * freqs + to_freq))
    return lax.ppermute(value, BOTH, route)


def search(spectra, channel_gain, bandpass_bin, drift_range, hit_cutoff):
    groups, integrations, chan_dev = spectra.shape
    sections, freqs = lax.axis_size("section"), lax.axis_size("freq")
    section, freq = lax.axis_index("section"), lax.axis_index("freq")
    total_bins = 4 * freqs
    bin_tiles = -(-total_bins // LANES)
    rates = hit_cutoff.shape[1]
    strides = rates // sections
    margin = rates * (integrations - 1)
    cols = chan_dev // LANES
    sizes = Sizes(groups, integrations, bin_tiles, margin, rates, strides)
    blocks = integrations // SUBS
    assert cols % SUBS == 0 and integrations % SUBS == 0 and margin <= LANES - SUBS
    assert sections > 1 and groups * cols == LANES and integrations <= cols
    assert freqs % 2 == 0 and 2 * groups + 1 <= SUBS - 2 and rates % sections == 0
    x = spectra.reshape(groups, blocks, SUBS, cols, LANES).transpose(0, 1, 3, 2, 4)
    x = x.reshape(groups * blocks * cols * SUBS, LANES)
    gain = channel_gain.reshape(cols, LANES)
    bins = bandpass_bin.reshape(cols, LANES)
    shape = functools.partial(jax.ShapeDtypeStruct, dtype=jnp.float32)
    side, _ = pack_count(margin)
    rim_tiles = -(-groups * blocks // side)

    packed, x_near, gain_near, bins_near = pl.pallas_call(
        functools.partial(bin_kernel, groups, integrations, bin_tiles, margin),
        out_shape=(
            shape(((2 * bin_tiles + rim_tiles) * SUBS, LANES)),
            shape(x.shape),
            shape(gain.shape),
            jax.ShapeDtypeStruct(bins.shape, bins.dtype),
        ),
        in_specs=[HBM] * 3,
        out_specs=(VMEM,) * 4,
        scratch_shapes=[pltpu.SemaphoreType.DMA((2 + groups,))],
        compiler_params=PARAMS,
        name="bin_sums",
    )(far(x), far(gain), far(bins))

    turned, cuts = pl.pallas_call(
        functools.partial(turn_kernel, groups, integrations),
        out_shape=(shape((integrations * LANES, LANES)), shape((rates * integrations, LANES))),
        in_specs=[VMEM, HBM, HBM],
        out_specs=(VMEM, VMEM),
        scratch_shapes=[
            pltpu.SMEM(hit_cutoff.shape, jnp.int32),
            pltpu.SMEM(drift_range.shape, jnp.int32),
            pltpu.SemaphoreType.DMA((2,)),
        ],
        compiler_params=PARAMS,
        cost_estimate=pl.CostEstimate(flops=10**7, bytes_accessed=0, transcendentals=0),
        name="turn",
    )(x_near, far(hit_cutoff), far(drift_range))

    mate = lambda s, f: (s, f ^ 1)

    def across(s, f):
        other = f + 1 if f % 2 else f - 1
        if 0 <= other < freqs:
            return (s, other)
        return (s ^ 1, f) if sections % 2 == 0 else (s, f)

    rows = bin_tiles * SUBS
    from_mate = swap(packed, mate)
    pairs = packed[: 2 * rows] + from_mate[: 2 * rows]
    pair, shifted_pair = pairs[:rows], pairs[rows:]
    to_across = jnp.concatenate([pair, packed[2 * rows :]], axis=0)
    to_across, shifted_pair = lax.optimization_barrier((to_across, shifted_pair))
    from_across = swap(to_across, across)
    has_across = jnp.logical_and(freq != 0, freq != freqs - 1)
    own = pair + jnp.where(has_across, from_across[:rows], 0.0)
    if sections == 2:

        def across_other(s, f):
            return (1, across(s, f)[1]) if s == 0 else (0, f ^ 1)

        beside = swap(shifted_pair, lambda s, f: (1 - s, f))
        beside_across = swap(shifted_pair, across_other)
        earlier = beside + jnp.where(has_across, beside_across, 0.0)
        own = own + jnp.where(section == 1, earlier, 0.0)
    else:
        all_shifted = lax.all_gather(shifted_pair, "section")
        is_earlier = lax.broadcasted_iota(jnp.int32, (sections, 1, 1), 0) < section
        earlier = jnp.sum(jnp.where(is_earlier, all_shifted, 0.0), axis=0)
        earlier_across = swap(earlier, across)
        own = own + earlier + jnp.where(has_across, earlier_across, 0.0)
    odd = freq % 2 == 1
    following = jnp.where(odd, own, swap(own, mate))
    next_rim = jnp.where(odd, from_across[rows:], from_mate[2 * rows :])
    next_bins = jnp.where(odd, from_across[SUBS - 2 : SUBS - 1], from_mate[SUBS - 1 : SUBS])

    def work(flops):
        return pl.CostEstimate(flops=flops, bytes_accessed=0, transcendentals=0)

    def later(span):
        half = pltpu.VMEM((integrations // 2 * span, LANES), jnp.float32)
        return [half] * (integrations.bit_length() - 2)

    normal, half_tail, rim_index, head = pl.pallas_call(
        functools.partial(main_kernel, sizes),
        out_shape=(
            shape((integrations * sizes.main_span, LANES)),
            shape((integrations * sizes.tail_span, LANES)),
            jax.ShapeDtypeStruct((sizes.extra, LANES), jnp.int32),
            shape((strides * sizes.head, LANES)),
        ),
        in_specs=[VMEM] * 7,
        out_specs=(VMEM,) * 4,
        scratch_shapes=later(sizes.main_span),
        compiler_params=PARAMS,
        cost_estimate=work(10**7),
        name="main",
    )(gain_near, bins_near, own, next_bins, next_rim, turned, cuts)
    scores_shape = shape((groups * strides * cols, LANES))
    tail, first_scores = pl.pallas_call(
        functools.partial(rim_kernel, sizes),
        out_shape=(shape(half_tail.shape), scores_shape),
        in_specs=[VMEM] * 5,
        out_specs=(VMEM, VMEM),
        scratch_shapes=later(sizes.tail_span),
        compiler_params=PARAMS,
        name="rim",
    )(following, rim_index, half_tail, head, cuts)

    def scores(hop):
        return pl.pallas_call(
            functools.partial(tree_kernel, sizes, hop),
            out_shape=scores_shape,
            in_specs=[VMEM] * 3,
            out_specs=VMEM,
            scratch_shapes=later(sizes.main_span) + later(sizes.tail_span),
            compiler_params=PARAMS,
            cost_estimate=work(10**7),
            name="tree",
        )(normal, tail, cuts)

    arrived = []
    for hop in range(1, sections):
        sent = first_scores if hop == 1 else scores(hop)
        arrived.append(swap(sent, lambda s, f: ((s + hop) % sections, f)))
    out_shape = shape((sections * groups * strides * cols, LANES))
    out = pl.pallas_call(
        functools.partial(own_kernel, sizes),
        out_shape=out_shape,
        in_specs=[VMEM] * 3,
        out_specs=HBM,
        scratch_shapes=[pltpu.VMEM(scores_shape.shape, jnp.float32), pltpu.SemaphoreType.DMA]
        + later(sizes.main_span)
        + later(sizes.tail_span),
        compiler_params=PARAMS,
        cost_estimate=work(10**7),
        name="own",
    )(normal, tail, cuts)
    for hop, part in enumerate(arrived, 1):
        out = pl.pallas_call(
            functools.partial(place_kernel, hop),
            out_shape=out_shape,
            in_specs=[VMEM, HBM],
            out_specs=HBM,
            scratch_shapes=[pltpu.SemaphoreType.DMA],
            input_output_aliases={1: 0},
            compiler_params=PARAMS,
            name="place",
        )(part, far(out))
    return out.reshape(sections * groups, strides, chan_dev)


def solution(mesh):
    return jax.shard_map(
        search,
        mesh=mesh,
        in_specs=(P("section", None, "freq"), P("freq"), P("freq"), P(), P()),
        out_specs=P(None, "section", "freq"),
        check_vma=False,
    )
```

```python
import dataclasses
import functools

import jax
import jax.numpy as jnp
from jax import lax
from jax.experimental import pallas as pl
from jax.experimental.pallas import tpu as pltpu
from jax.sharding import PartitionSpec as P


LANES = 128
SUBS = 8
BOTH = ("section", "freq")
CHUNK = 8
NEVER = 3e38
VMEM = pl.BlockSpec(memory_space=pltpu.VMEM)
SMEM = pl.BlockSpec(memory_space=pltpu.SMEM)
HBM = pl.BlockSpec(memory_space=pltpu.HBM)
PARAMS = pltpu.CompilerParams(vmem_limit_bytes=16 * 2**20)


@dataclasses.dataclass(frozen=True)
class Sizes:
    groups: int
    integrations: int
    bin_tiles: int
    margin: int
    rates: int
    strides: int

    @property
    def extra(self):
        return -(-self.margin // SUBS) * SUBS + SUBS

    @property
    def head(self):
        return LANES - -(-self.margin // SUBS) * SUBS

    @property
    def main_span(self):
        return LANES + SUBS

    @property
    def tail_span(self):
        return LANES - self.head + self.extra


def lane_iota():
    return lax.broadcasted_iota(jnp.int32, (SUBS, LANES), 1)


def row_iota():
    return lax.broadcasted_iota(jnp.int32, (SUBS, LANES), 0)


def spectra_rows(x_ref, group, t, first, rows, cols, integrations):
    block = group * (integrations // SUBS) + t // SUBS
    return x_ref[pl.ds((block * cols + first) * SUBS + t % SUBS, rows, stride=SUBS), :]


def pack_count(margin):
    room = 1 << (margin - 1).bit_length()
    return LANES // room, room


def bin_kernel(
    groups,
    integrations,
    bin_tiles,
    margin,
    x_hbm,
    gain_hbm,
    bins_hbm,
    packed_ref,
    x_ref,
    gain_ref,
    bins_ref,
    sems,
):
    cols = gain_ref.shape[0]
    tiles = cols // SUBS
    group_rows = integrations * cols
    copies = [
        pltpu.make_async_copy(bins_hbm, bins_ref, sems.at[0]),
        pltpu.make_async_copy(gain_hbm, gain_ref, sems.at[1]),
    ]
    for group in range(groups):
        part = pl.ds(group * group_rows, group_rows)
        copies.append(pltpu.make_async_copy(x_hbm.at[part], x_ref.at[part], sems.at[2 + group]))
    for copy in copies:
        copy.start()
    lane, row = lane_iota(), row_iota()
    copies[0].wait()
    bins = [bins_ref[tile * SUBS : (tile + 1) * SUBS, :] for tile in range(tiles)]
    first, last = jnp.min(bins[0]), jnp.max(bins[-1])
    copies[1].wait()
    summed, rims = [], []
    for group in range(groups):
        copies[2 + group].wait()
        for block in range(integrations // SUBS):
            at = (group * (integrations // SUBS) + block) * cols * SUBS
            rims.append(x_ref[at : at + SUBS, :] * gain_ref[0:1, :])
        for tile in range(tiles):
            parts = [
                spectra_rows(x_ref, group, t, tile * SUBS, SUBS, cols, integrations)
                for t in range(integrations)
            ]
            while len(parts) > 1:
                parts = [a + b for a, b in zip(parts[0::2], parts[1::2])]
            summed.append(parts[0] * gain_ref[tile * SUBS : (tile + 1) * SUBS, :])
    side, room = pack_count(margin)
    for at in range(0, len(rims), side):
        packed = rims[at]
        for place, rim in enumerate(rims[at + 1 : at + side], 1):
            packed = jnp.where(lane // room == place, pltpu.roll(rim, place * room, 1), packed)
        to = 2 * bin_tiles * SUBS + at // side * SUBS
        packed_ref[to : to + SUBS, :] = packed

    def some_bins(step, tables):
        for u in range(CHUNK):
            b = first + step * CHUNK + u
            masks = [part == b for part in bins]
            stacked = jnp.zeros((SUBS, LANES), jnp.float32)
            for quantity in range(groups + 1):
                partial = jnp.zeros((SUBS, LANES), jnp.float32)
                for tile in range(tiles):
                    value = 1.0 if quantity == groups else summed[quantity * tiles + tile]
                    partial = partial + jnp.where(masks[tile], value, 0.0)
                stacked = jnp.where(row == quantity, jnp.sum(partial, axis=0, keepdims=True), stacked)
            total = jnp.sum(stacked, axis=1, keepdims=True)
            tables = tuple(
                table + jnp.where(lane == b - q * LANES, total, 0.0) for q, table in enumerate(tables)
            )
        return tables

    start = tuple(jnp.zeros((SUBS, LANES), jnp.float32) for _ in range(bin_tiles))
    tables = lax.fori_loop(0, (last - first) // CHUNK + 1, some_bins, start)
    rim_bins = jnp.broadcast_to(bins_ref[0:1, :].astype(jnp.float32), (SUBS, LANES))
    rim_bins_row = SUBS - 2 + lax.rem(lax.axis_index("freq"), 2)
    for q, table in enumerate(tables):
        shifted = pltpu.roll(table, groups + 1, 0)
        packed_ref[(bin_tiles + q) * SUBS : (bin_tiles + q + 1) * SUBS, :] = jnp.where(
            (row > groups) & (row <= 2 * groups), shifted, 0.0
        )
        if q == 0:
            table = jnp.where(row == rim_bins_row, rim_bins, table)
        packed_ref[q * SUBS : (q + 1) * SUBS, :] = table


def turn_kernel(groups, integrations, x_ref, cut_hbm, reach_hbm, turned_ref, cuts_ref, cut_ref, reach_ref, sems):
    copies = [
        pltpu.make_async_copy(cut_hbm, cut_ref, sems.at[0]),
        pltpu.make_async_copy(reach_hbm, reach_ref, sems.at[1]),
    ]
    for copy in copies:
        copy.start()
    cols = LANES // groups
    for t in range(integrations):
        block = jnp.concatenate(
            [spectra_rows(x_ref, group, t, 0, cols, cols, integrations) for group in range(groups)], axis=0
        )
        turned_ref[t * LANES : (t + 1) * LANES, :] = block.T
    for copy in copies:
        copy.wait()
    lane = lax.broadcasted_iota(jnp.int32, (1, LANES), 1)
    section = lax.axis_index("section")
    for index in range(cut_ref.shape[1]):
        for drift in range(integrations):
            line = jnp.zeros((1, LANES), jnp.float32)
            for group in range(groups):
                group_id = section * groups + group
                cut = cut_ref[group_id, index, drift].astype(jnp.float32) * (4.0 / 256.0)
                cut = jnp.where(index + 1 <= reach_ref[group_id], cut, NEVER)
                line = jnp.where(lane // cols == group, cut, line)
            at = index * integrations + drift
            cuts_ref[at : at + 1, :] = line


def look_up(rows, bins):
    found = None
    for q, values in enumerate(rows):
        spread = jnp.broadcast_to(values, bins.shape)
        index = bins if len(rows) == 1 else jnp.clip(bins - q * LANES, 0, LANES - 1)
        value = jnp.take_along_axis(spread, index, axis=1)
        found = value if q == 0 else jnp.where(bins >= q * LANES, value, found)
    return found


def inverse_levels(groups, integrations, bin_tiles, table_ref):
    first = lax.axis_index("section") * groups
    result = [[] for _ in range(groups)]
    for q in range(bin_tiles):
        rows = [table_ref[q * SUBS + r : q * SUBS + r + 1, :] for r in range(2 * groups + 1)]
        running = sum(rows[groups + 2 :], rows[groups + 1])
        for group in range(groups):
            running = running + rows[group]
            tally = rows[groups] * ((first + group + 1) * integrations).astype(jnp.float32)
            result[group].append(tally / running)
    return result


def main_kernel(
    sizes,
    gain_ref,
    bins_ref,
    own_ref,
    rim_bins_ref,
    rim_ref,
    turned_ref,
    cuts_ref,
    normal_ref,
    tail_ref,
    rim_index_ref,
    head_ref,
    *later_refs,
):
    groups, integrations = sizes.groups, sizes.integrations
    tiles = gain_ref.shape[0] // SUBS
    inverse = inverse_levels(groups, integrations, sizes.bin_tiles, own_ref)
    factors = []
    for group in range(groups):
        for tile in range(tiles):
            part = slice(tile * SUBS, (tile + 1) * SUBS)
            factors.append(look_up(inverse[group], bins_ref[part, :]) * gain_ref[part, :])
    factor = jnp.concatenate(factors, axis=0).T
    cols = LANES // groups
    side, room = pack_count(sizes.margin)
    rims = []
    for group in range(groups):
        for block in range(integrations // SUBS):
            at = group * (integrations // SUBS) + block
            rim = rim_ref[at // side * SUBS : (at // side + 1) * SUBS, :]
            rims.append(pltpu.roll(rim, LANES - at % side * room, 1) if at % side else rim)
        rims.append(jnp.zeros((cols - integrations, LANES), jnp.float32))
    raw = jnp.concatenate(rims, axis=0).T[: sizes.extra]
    rim_index = jnp.broadcast_to(rim_bins_ref[0:1, :], (LANES, LANES)).T
    rim_index_ref[...] = rim_index[: sizes.extra].astype(jnp.int32)
    last_col = lax.broadcasted_iota(jnp.int32, (sizes.extra, LANES), 1) % cols == cols - 1
    for t in range(integrations):
        normal = turned_ref[t * LANES : (t + 1) * LANES, :] * factor - 1.0
        at = t * sizes.main_span
        normal_ref[at : at + LANES, :] = normal
        normal_ref[at + LANES : at + sizes.main_span, :] = jnp.zeros((sizes.main_span - LANES, LANES), jnp.float32)
        at = t * sizes.tail_span
        tail_ref[at : at + LANES - sizes.head, :] = normal[sizes.head :]
        outer = pltpu.roll(raw, cols - 1 - t, 1) if cols - 1 - t else raw
        tail_ref[at + LANES - sizes.head : at + sizes.tail_span, :] = jnp.where(
            last_col, outer, pltpu.roll(normal[: sizes.extra], LANES - 1, 1)
        )
    for index in range(sizes.strides):
        scores = tree(sizes, 1, index, normal_ref, sizes.main_span, sizes.head, cuts_ref, later_refs)
        head_ref[index * sizes.head : (index + 1) * sizes.head, :] = scores


def rim_kernel(
    sizes, own_ref, mate_ref, rim_index_ref, half_tail_ref, head_ref, cuts_ref, tail_ref, out_ref, *later_refs
):
    groups, integrations = sizes.groups, sizes.integrations
    cols = LANES // groups
    lane = lane_iota()
    at_end = lax.axis_index("freq") == lax.axis_size("freq") - 1
    last_col = lane % cols == cols - 1
    odd = lax.rem(lax.axis_index("freq"), 2) == 1
    table = jnp.where(odd, own_ref[...], mate_ref[...])
    inverse = inverse_levels(groups, integrations, sizes.bin_tiles, table)
    inner = LANES - sizes.head
    for row in range(0, sizes.extra - SUBS, SUBS):
        index = rim_index_ref[row : row + SUBS, :]
        level = look_up(inverse[0], index)
        for group in range(1, groups):
            level = jnp.where(lane // cols == group, look_up(inverse[group], index), level)
        for t in range(integrations):
            at = t * sizes.tail_span + inner + row
            half = half_tail_ref[at : at + SUBS, :]
            edge = jnp.where(at_end, 0.0, half * level - 1.0)
            tail_ref[at : at + SUBS, :] = jnp.where(last_col, edge, half)
    for index in range(sizes.strides):
        head = head_ref[index * sizes.head : (index + 1) * sizes.head, :]
        rest = tree(sizes, 1, index, tail_ref, sizes.tail_span, LANES - sizes.head, cuts_ref, later_refs)
        put_scores(sizes, out_ref, index, [head, rest])


def tree_kernel(sizes, hop, normal_ref, tail_ref, cuts_ref, out_ref, *later_refs):
    half = len(later_refs) // 2
    for index in range(sizes.strides):
        head = tree(sizes, hop, index, normal_ref, sizes.main_span, sizes.head, cuts_ref, later_refs[:half])
        rest = tree(
            sizes, hop, index, tail_ref, sizes.tail_span, LANES - sizes.head, cuts_ref, later_refs[half:]
        )
        put_scores(sizes, out_ref, index, [head, rest])


def own_kernel(sizes, normal_ref, tail_ref, cuts_ref, out_hbm, scores_ref, sem, *later_refs):
    tree_kernel(sizes, 0, normal_ref, tail_ref, cuts_ref, scores_ref, *later_refs)
    rows = scores_ref.shape[0]
    at = pl.multiple_of(lax.axis_index("section") * rows, SUBS)
    copy = pltpu.make_async_copy(scores_ref, out_hbm.at[pl.ds(at, rows)], sem)
    copy.start()
    copy.wait()


def place_kernel(hop, scores_ref, _, out_hbm, sem):
    rows, sections = scores_ref.shape[0], lax.axis_size("section")
    at = pl.multiple_of(lax.rem(lax.axis_index("section") + sections - hop, sections) * rows, SUBS)
    copy = pltpu.make_async_copy(scores_ref, out_hbm.at[pl.ds(at, rows)], sem)
    copy.start()
    copy.wait()


def put_scores(sizes, out_ref, index, parts):
    scores = jnp.concatenate(parts, axis=0).T
    cols = LANES // sizes.groups
    for group in range(sizes.groups):
        at = (group * sizes.strides + index) * cols
        out_ref[at : at + cols, :] = scores[group * cols : (group + 1) * cols]


def tree(sizes, hop, index, normal_ref, span, length, cuts_ref, later_refs):
    integrations = sizes.integrations
    levels = integrations.bit_length() - 1
    target = lax.rem(lax.axis_index("section") + hop, lax.axis_size("section"))
    stride = target * sizes.strides + index + 1

    def values(level, block, at):
        if level == 0:
            return [normal_ref[block * span + at : block * span + at + SUBS, :]]
        former = values(level - 1, 2 * block, at)
        rows = 2 ** (level - 1)
        result = []
        for half, anchor in enumerate(former):
            if level == 1:
                ref, base = normal_ref, (2 * block + 1) * span
            else:
                ref, base = later_refs[level - 2], (block * rows + half) * span
            for steps in (half, half + 1):
                result.append(anchor + ref[pl.ds(base + at + steps * stride, SUBS), :])
        return result

    for level in range(1, levels):
        reach = min(span, length + -(-(integrations - 2**level) * sizes.rates // SUBS) * SUBS)
        reach = min(reach, span - SUBS)
        for block in range(1, integrations >> level, 2):
            for at in range(0, reach, SUBS):
                for drift, value in enumerate(values(level, block, at)):
                    row = ((block // 2) * 2**level + drift) * span + at
                    later_refs[level - 1][row : row + SUBS, :] = value
    parts = []
    for at in range(0, length, SUBS):
        score = jnp.zeros((SUBS, LANES), jnp.float32)
        for drift, value in enumerate(values(levels, 0, at)):
            cut = cuts_ref[pl.ds((stride - 1) * integrations + drift, 1), :]
            score = score + jnp.maximum(value - cut, 0.0)
        parts.append(score * (0.25 / integrations))
    return jnp.concatenate(parts, axis=0)


def far(value):
    return pltpu.with_memory_space_constraint(value, pltpu.HBM)


def swap(value, partner):
    sections, freqs = lax.axis_size("section"), lax.axis_size("freq")
    route = []
    for section in range(sections):
        for freq in range(freqs):
            to_section, to_freq = partner(section, freq)
            route.append((section * freqs + freq, to_section * freqs + to_freq))
    return lax.ppermute(value, BOTH, route)


def search(spectra, channel_gain, bandpass_bin, drift_range, hit_cutoff):
    groups, integrations, chan_dev = spectra.shape
    sections, freqs = lax.axis_size("section"), lax.axis_size("freq")
    section, freq = lax.axis_index("section"), lax.axis_index("freq")
    total_bins = 4 * freqs
    bin_tiles = -(-total_bins // LANES)
    rates = hit_cutoff.shape[1]
    strides = rates // sections
    margin = rates * (integrations - 1)
    cols = chan_dev // LANES
    sizes = Sizes(groups, integrations, bin_tiles, margin, rates, strides)
    blocks = integrations // SUBS
    assert cols % SUBS == 0 and integrations % SUBS == 0 and margin <= LANES - SUBS
    assert sections > 1 and groups * cols == LANES and integrations <= cols
    assert freqs % 2 == 0 and 2 * groups + 1 <= SUBS - 2 and rates % sections == 0
    x = spectra.reshape(groups, blocks, SUBS, cols, LANES).transpose(0, 1, 3, 2, 4)
    x = x.reshape(groups * blocks * cols * SUBS, LANES)
    gain = channel_gain.reshape(cols, LANES)
    bins = bandpass_bin.reshape(cols, LANES)
    shape = functools.partial(jax.ShapeDtypeStruct, dtype=jnp.float32)
    side, _ = pack_count(margin)
    rim_tiles = -(-groups * blocks // side)

    packed, x_near, gain_near, bins_near = pl.pallas_call(
        functools.partial(bin_kernel, groups, integrations, bin_tiles, margin),
        out_shape=(
            shape(((2 * bin_tiles + rim_tiles) * SUBS, LANES)),
            shape(x.shape),
            shape(gain.shape),
            jax.ShapeDtypeStruct(bins.shape, bins.dtype),
        ),
        in_specs=[HBM] * 3,
        out_specs=(VMEM,) * 4,
        scratch_shapes=[pltpu.SemaphoreType.DMA((2 + groups,))],
        compiler_params=PARAMS,
        name="bin_sums",
    )(far(x), far(gain), far(bins))

    turned, cuts = pl.pallas_call(
        functools.partial(turn_kernel, groups, integrations),
        out_shape=(shape((integrations * LANES, LANES)), shape((rates * integrations, LANES))),
        in_specs=[VMEM, HBM, HBM],
        out_specs=(VMEM, VMEM),
        scratch_shapes=[
            pltpu.SMEM(hit_cutoff.shape, jnp.int32),
            pltpu.SMEM(drift_range.shape, jnp.int32),
            pltpu.SemaphoreType.DMA((2,)),
        ],
        compiler_params=PARAMS,
        cost_estimate=pl.CostEstimate(flops=10**7, bytes_accessed=0, transcendentals=0),
        name="turn",
    )(x_near, far(hit_cutoff), far(drift_range))

    mate = lambda s, f: (s, f ^ 1)

    def across(s, f):
        other = f + 1 if f % 2 else f - 1
        if 0 <= other < freqs:
            return (s, other)
        return (s ^ 1, f) if sections % 2 == 0 else (s, f)

    rows = bin_tiles * SUBS
    from_mate = swap(packed, mate)
    pairs = packed[: 2 * rows] + from_mate[: 2 * rows]
    pair, shifted_pair = pairs[:rows], pairs[rows:]
    to_across = jnp.concatenate([pair, packed[2 * rows :]], axis=0)
    to_across, shifted_pair = lax.optimization_barrier((to_across, shifted_pair))
    from_across = swap(to_across, across)
    has_across = jnp.logical_and(freq != 0, freq != freqs - 1)
    own = pair + jnp.where(has_across, from_across[:rows], 0.0)
    if sections == 2:

        def across_other(s, f):
            return (1, across(s, f)[1]) if s == 0 else (0, f ^ 1)

        beside = swap(shifted_pair, lambda s, f: (1 - s, f))
        beside_across = swap(shifted_pair, across_other)
        earlier = beside + jnp.where(has_across, beside_across, 0.0)
        own = own + jnp.where(section == 1, earlier, 0.0)
    else:
        all_shifted = lax.all_gather(shifted_pair, "section")
        is_earlier = lax.broadcasted_iota(jnp.int32, (sections, 1, 1), 0) < section
        earlier = jnp.sum(jnp.where(is_earlier, all_shifted, 0.0), axis=0)
        earlier_across = swap(earlier, across)
        own = own + earlier + jnp.where(has_across, earlier_across, 0.0)
    odd = freq % 2 == 1
    mate_table = swap(own, mate)
    next_rim = jnp.where(odd, from_across[rows:], from_mate[2 * rows :])
    next_bins = jnp.where(odd, from_across[SUBS - 2 : SUBS - 1], from_mate[SUBS - 1 : SUBS])

    def work(flops):
        return pl.CostEstimate(flops=flops, bytes_accessed=0, transcendentals=0)

    def later(span):
        half = pltpu.VMEM((integrations // 2 * span, LANES), jnp.float32)
        return [half] * (integrations.bit_length() - 2)

    normal, half_tail, rim_index, head = pl.pallas_call(
        functools.partial(main_kernel, sizes),
        out_shape=(
            shape((integrations * sizes.main_span, LANES)),
            shape((integrations * sizes.tail_span, LANES)),
            jax.ShapeDtypeStruct((sizes.extra, LANES), jnp.int32),
            shape((strides * sizes.head, LANES)),
        ),
        in_specs=[VMEM] * 7,
        out_specs=(VMEM,) * 4,
        scratch_shapes=later(sizes.main_span),
        compiler_params=PARAMS,
        cost_estimate=work(10**7),
        name="main",
    )(gain_near, bins_near, own, next_bins, next_rim, turned, cuts)
    scores_shape = shape((groups * strides * cols, LANES))
    tail, first_scores = pl.pallas_call(
        functools.partial(rim_kernel, sizes),
        out_shape=(shape(half_tail.shape), scores_shape),
        in_specs=[VMEM] * 6,
        input_output_aliases={3: 0},
        out_specs=(VMEM, VMEM),
        scratch_shapes=later(sizes.tail_span),
        compiler_params=PARAMS,
        name="rim",
    )(own, mate_table, rim_index, half_tail, head, cuts)

    def scores(hop):
        return pl.pallas_call(
            functools.partial(tree_kernel, sizes, hop),
            out_shape=scores_shape,
            in_specs=[VMEM] * 3,
            out_specs=VMEM,
            scratch_shapes=later(sizes.main_span) + later(sizes.tail_span),
            compiler_params=PARAMS,
            cost_estimate=work(10**7),
            name="tree",
        )(normal, tail, cuts)

    arrived = []
    for hop in range(1, sections):
        sent = first_scores if hop == 1 else scores(hop)
        arrived.append(swap(sent, lambda s, f: ((s + hop) % sections, f)))
    out_shape = shape((sections * groups * strides * cols, LANES))
    out = pl.pallas_call(
        functools.partial(own_kernel, sizes),
        out_shape=out_shape,
        in_specs=[VMEM] * 3,
        out_specs=HBM,
        scratch_shapes=[pltpu.VMEM(scores_shape.shape, jnp.float32), pltpu.SemaphoreType.DMA]
        + later(sizes.main_span)
        + later(sizes.tail_span),
        compiler_params=PARAMS,
        cost_estimate=work(10**7),
        name="own",
    )(normal, tail, cuts)
    for hop, part in enumerate(arrived, 1):
        out = pl.pallas_call(
            functools.partial(place_kernel, hop),
            out_shape=out_shape,
            in_specs=[VMEM, HBM],
            out_specs=HBM,
            scratch_shapes=[pltpu.SemaphoreType.DMA],
            input_output_aliases={1: 0},
            compiler_params=PARAMS,
            name="place",
        )(part, far(out))
    return out.reshape(sections * groups, strides, chan_dev)


def solution(mesh):
    return jax.shard_map(
        search,
        mesh=mesh,
        in_specs=(P("section", None, "freq"), P("freq"), P("freq"), P(), P()),
        out_specs=P(None, "section", "freq"),
        check_vma=False,
    )
```

```python
import dataclasses
import functools

import jax
import jax.numpy as jnp
from jax import lax
from jax.experimental import pallas as pl
from jax.experimental.pallas import tpu as pltpu
from jax.sharding import PartitionSpec as P


LANES = 128
SUBS = 8
BOTH = ("section", "freq")
CHUNK = 8
NEVER = 3e38
VMEM = pl.BlockSpec(memory_space=pltpu.VMEM)
SMEM = pl.BlockSpec(memory_space=pltpu.SMEM)
HBM = pl.BlockSpec(memory_space=pltpu.HBM)
PARAMS = pltpu.CompilerParams(vmem_limit_bytes=16 * 2**20)


@dataclasses.dataclass(frozen=True)
class Sizes:
    groups: int
    integrations: int
    bin_tiles: int
    margin: int
    rates: int
    strides: int

    @property
    def extra(self):
        return -(-self.margin // SUBS) * SUBS + SUBS

    @property
    def head(self):
        return LANES - -(-self.margin // SUBS) * SUBS

    @property
    def main_span(self):
        return LANES + SUBS

    @property
    def tail_span(self):
        return LANES - self.head + self.extra


def lane_iota():
    return lax.broadcasted_iota(jnp.int32, (SUBS, LANES), 1)


def row_iota():
    return lax.broadcasted_iota(jnp.int32, (SUBS, LANES), 0)


def spectra_rows(x_ref, group, t, first, rows, cols, integrations):
    block = group * (integrations // SUBS) + t // SUBS
    return x_ref[pl.ds((block * cols + first) * SUBS + t % SUBS, rows, stride=SUBS), :]


def pack_count(margin):
    room = 1 << (margin - 1).bit_length()
    return LANES // room, room


def bin_kernel(
    groups,
    integrations,
    bin_tiles,
    margin,
    x_hbm,
    gain_hbm,
    bins_hbm,
    packed_ref,
    x_ref,
    gain_ref,
    bins_ref,
    sems,
):
    cols = gain_ref.shape[0]
    tiles = cols // SUBS
    group_rows = integrations * cols
    copies = [
        pltpu.make_async_copy(bins_hbm, bins_ref, sems.at[0]),
        pltpu.make_async_copy(gain_hbm, gain_ref, sems.at[1]),
    ]
    for group in range(groups):
        part = pl.ds(group * group_rows, group_rows)
        copies.append(pltpu.make_async_copy(x_hbm.at[part], x_ref.at[part], sems.at[2 + group]))
    for copy in copies:
        copy.start()
    lane, row = lane_iota(), row_iota()
    copies[0].wait()
    bins = [bins_ref[tile * SUBS : (tile + 1) * SUBS, :] for tile in range(tiles)]
    first, last = jnp.min(bins[0]), jnp.max(bins[-1])
    copies[1].wait()
    summed, rims = [], []
    for group in range(groups):
        copies[2 + group].wait()
        for block in range(integrations // SUBS):
            at = (group * (integrations // SUBS) + block) * cols * SUBS
            rims.append(x_ref[at : at + SUBS, :] * gain_ref[0:1, :])
        for tile in range(tiles):
            parts = [
                spectra_rows(x_ref, group, t, tile * SUBS, SUBS, cols, integrations)
                for t in range(integrations)
            ]
            while len(parts) > 1:
                parts = [a + b for a, b in zip(parts[0::2], parts[1::2])]
            summed.append(parts[0] * gain_ref[tile * SUBS : (tile + 1) * SUBS, :])
    side, room = pack_count(margin)
    for at in range(0, len(rims), side):
        packed = rims[at]
        for place, rim in enumerate(rims[at + 1 : at + side], 1):
            packed = jnp.where(lane // room == place, pltpu.roll(rim, place * room, 1), packed)
        to = 2 * bin_tiles * SUBS + at // side * SUBS
        packed_ref[to : to + SUBS, :] = packed

    def some_bins(step, tables):
        for u in range(CHUNK):
            b = first + step * CHUNK + u
            masks = [part == b for part in bins]
            stacked = jnp.zeros((SUBS, LANES), jnp.float32)
            for quantity in range(groups + 1):
                partial = jnp.zeros((SUBS, LANES), jnp.float32)
                for tile in range(tiles):
                    value = 1.0 if quantity == groups else summed[quantity * tiles + tile]
                    partial = partial + jnp.where(masks[tile], value, 0.0)
                stacked = jnp.where(row == quantity, jnp.sum(partial, axis=0, keepdims=True), stacked)
            total = jnp.sum(stacked, axis=1, keepdims=True)
            tables = tuple(
                table + jnp.where(lane == b - q * LANES, total, 0.0) for q, table in enumerate(tables)
            )
        return tables

    start = tuple(jnp.zeros((SUBS, LANES), jnp.float32) for _ in range(bin_tiles))
    tables = lax.fori_loop(0, (last - first) // CHUNK + 1, some_bins, start)
    rim_bins = jnp.broadcast_to(bins_ref[0:1, :].astype(jnp.float32), (SUBS, LANES))
    rim_bins_row = SUBS - 2 + lax.rem(lax.axis_index("freq"), 2)
    for q, table in enumerate(tables):
        shifted = pltpu.roll(table, groups + 1, 0)
        packed_ref[(bin_tiles + q) * SUBS : (bin_tiles + q + 1) * SUBS, :] = jnp.where(
            (row > groups) & (row <= 2 * groups), shifted, 0.0
        )
        if q == 0:
            table = jnp.where(row == rim_bins_row, rim_bins, table)
        packed_ref[q * SUBS : (q + 1) * SUBS, :] = table


def turn_kernel(groups, integrations, x_ref, cut_hbm, reach_hbm, turned_ref, cuts_ref, cut_ref, reach_ref, sems):
    copies = [
        pltpu.make_async_copy(cut_hbm, cut_ref, sems.at[0]),
        pltpu.make_async_copy(reach_hbm, reach_ref, sems.at[1]),
    ]
    for copy in copies:
        copy.start()
    cols = LANES // groups
    for t in range(integrations):
        block = jnp.concatenate(
            [spectra_rows(x_ref, group, t, 0, cols, cols, integrations) for group in range(groups)], axis=0
        )
        turned_ref[t * LANES : (t + 1) * LANES, :] = block.T
    for copy in copies:
        copy.wait()
    lane = lax.broadcasted_iota(jnp.int32, (1, LANES), 1)
    section = lax.axis_index("section")
    for index in range(cut_ref.shape[1]):
        for drift in range(integrations):
            line = jnp.zeros((1, LANES), jnp.float32)
            for group in range(groups):
                group_id = section * groups + group
                cut = cut_ref[group_id, index, drift].astype(jnp.float32) * (4.0 / 256.0)
                cut = jnp.where(index + 1 <= reach_ref[group_id], cut, NEVER)
                line = jnp.where(lane // cols == group, cut, line)
            at = index * integrations + drift
            cuts_ref[at : at + 1, :] = line


def look_up(rows, bins):
    found = None
    for q, values in enumerate(rows):
        spread = jnp.broadcast_to(values, bins.shape)
        index = bins if len(rows) == 1 else jnp.clip(bins - q * LANES, 0, LANES - 1)
        value = jnp.take_along_axis(spread, index, axis=1)
        found = value if q == 0 else jnp.where(bins >= q * LANES, value, found)
    return found


def inverse_levels(groups, integrations, bin_tiles, table_ref):
    first = lax.axis_index("section") * groups
    result = [[] for _ in range(groups)]
    for q in range(bin_tiles):
        rows = [table_ref[q * SUBS + r : q * SUBS + r + 1, :] for r in range(2 * groups + 1)]
        running = sum(rows[groups + 2 :], rows[groups + 1])
        for group in range(groups):
            running = running + rows[group]
            tally = rows[groups] * ((first + group + 1) * integrations).astype(jnp.float32)
            result[group].append(tally / running)
    return result


def main_kernel(
    sizes,
    gain_ref,
    bins_ref,
    own_ref,
    rim_bins_ref,
    rim_ref,
    turned_ref,
    cuts_ref,
    normal_ref,
    tail_ref,
    rim_index_ref,
    head_ref,
    *later_refs,
):
    groups, integrations = sizes.groups, sizes.integrations
    tiles = gain_ref.shape[0] // SUBS
    inverse = inverse_levels(groups, integrations, sizes.bin_tiles, own_ref)
    factors = []
    for group in range(groups):
        for tile in range(tiles):
            part = slice(tile * SUBS, (tile + 1) * SUBS)
            factors.append(look_up(inverse[group], bins_ref[part, :]) * gain_ref[part, :])
    factor = jnp.concatenate(factors, axis=0).T
    cols = LANES // groups
    side, room = pack_count(sizes.margin)
    rims = []
    for group in range(groups):
        for block in range(integrations // SUBS):
            at = group * (integrations // SUBS) + block
            rim = rim_ref[at // side * SUBS : (at // side + 1) * SUBS, :]
            rims.append(pltpu.roll(rim, LANES - at % side * room, 1) if at % side else rim)
        rims.append(jnp.zeros((cols - integrations, LANES), jnp.float32))
    raw = jnp.concatenate(rims, axis=0).T[: sizes.extra]
    rim_index = jnp.broadcast_to(rim_bins_ref[0:1, :], (LANES, LANES)).T
    rim_index_ref[...] = rim_index[: sizes.extra].astype(jnp.int32)
    last_col = lax.broadcasted_iota(jnp.int32, (sizes.extra, LANES), 1) % cols == cols - 1
    for t in range(integrations):
        normal = turned_ref[t * LANES : (t + 1) * LANES, :] * factor - 1.0
        at = t * sizes.main_span
        normal_ref[at : at + LANES, :] = normal
        normal_ref[at + LANES : at + sizes.main_span, :] = jnp.zeros((sizes.main_span - LANES, LANES), jnp.float32)
        at = t * sizes.tail_span
        tail_ref[at : at + LANES - sizes.head, :] = normal[sizes.head :]
        outer = pltpu.roll(raw, cols - 1 - t, 1) if cols - 1 - t else raw
        tail_ref[at + LANES - sizes.head : at + sizes.tail_span, :] = jnp.where(
            last_col, outer, pltpu.roll(normal[: sizes.extra], LANES - 1, 1)
        )
    for index in range(sizes.strides):
        scores = tree(sizes, 1, index, normal_ref, sizes.main_span, sizes.head, cuts_ref, later_refs)
        head_ref[index * sizes.head : (index + 1) * sizes.head, :] = scores


def rim_kernel(
    sizes, next_ref, rim_index_ref, half_tail_ref, head_ref, cuts_ref, tail_ref, out_ref, *later_refs
):
    groups, integrations = sizes.groups, sizes.integrations
    cols = LANES // groups
    lane = lane_iota()
    at_end = lax.axis_index("freq") == lax.axis_size("freq") - 1
    last_col = lane % cols == cols - 1
    inverse = inverse_levels(groups, integrations, sizes.bin_tiles, next_ref)
    inner = LANES - sizes.head
    for row in range(0, sizes.extra, SUBS):
        index = rim_index_ref[row : row + SUBS, :]
        level = look_up(inverse[0], index)
        for group in range(1, groups):
            level = jnp.where(lane // cols == group, look_up(inverse[group], index), level)
        for t in range(integrations):
            at = t * sizes.tail_span + inner + row
            half = half_tail_ref[at : at + SUBS, :]
            edge = jnp.where(at_end, 0.0, half * level - 1.0)
            tail_ref[at : at + SUBS, :] = jnp.where(last_col, edge, half)
    for t in range(integrations):
        at = t * sizes.tail_span
        tail_ref[at : at + inner, :] = half_tail_ref[at : at + inner, :]
    for index in range(sizes.strides):
        head = head_ref[index * sizes.head : (index + 1) * sizes.head, :]
        rest = tree(sizes, 1, index, tail_ref, sizes.tail_span, LANES - sizes.head, cuts_ref, later_refs)
        put_scores(sizes, out_ref, index, [head, rest])


def tree_kernel(sizes, hop, normal_ref, tail_ref, cuts_ref, out_ref, *later_refs):
    half = len(later_refs) // 2
    for index in range(sizes.strides):
        head = tree(sizes, hop, index, normal_ref, sizes.main_span, sizes.head, cuts_ref, later_refs[:half])
        rest = tree(
            sizes, hop, index, tail_ref, sizes.tail_span, LANES - sizes.head, cuts_ref, later_refs[half:]
        )
        put_scores(sizes, out_ref, index, [head, rest])


def put_scores(sizes, out_ref, index, parts):
    scores = jnp.concatenate(parts, axis=0).T
    cols = LANES // sizes.groups
    for group in range(sizes.groups):
        at = (group * sizes.strides + index) * cols
        out_ref[at : at + cols, :] = scores[group * cols : (group + 1) * cols]


def tree(sizes, hop, index, normal_ref, span, length, cuts_ref, later_refs):
    integrations = sizes.integrations
    levels = integrations.bit_length() - 1
    target = lax.rem(lax.axis_index("section") + hop, lax.axis_size("section"))
    stride = target * sizes.strides + index + 1

    def values(level, block, at):
        if level == 0:
            return [normal_ref[block * span + at : block * span + at + SUBS, :]]
        former = values(level - 1, 2 * block, at)
        rows = 2 ** (level - 1)
        result = []
        for half, anchor in enumerate(former):
            if level == 1:
                ref, base = normal_ref, (2 * block + 1) * span
            else:
                ref, base = later_refs[level - 2], (block * rows + half) * span
            for steps in (half, half + 1):
                result.append(anchor + ref[pl.ds(base + at + steps * stride, SUBS), :])
        return result

    for level in range(1, levels):
        reach = min(span, length + -(-(integrations - 2**level) * sizes.rates // SUBS) * SUBS)
        reach = min(reach, span - SUBS)
        for block in range(1, integrations >> level, 2):
            for at in range(0, reach, SUBS):
                for drift, value in enumerate(values(level, block, at)):
                    row = ((block // 2) * 2**level + drift) * span + at
                    later_refs[level - 1][row : row + SUBS, :] = value
    parts = []
    for at in range(0, length, SUBS):
        score = jnp.zeros((SUBS, LANES), jnp.float32)
        for drift, value in enumerate(values(levels, 0, at)):
            cut = cuts_ref[pl.ds((stride - 1) * integrations + drift, 1), :]
            score = score + jnp.maximum(value - cut, 0.0)
        parts.append(score * (0.25 / integrations))
    return jnp.concatenate(parts, axis=0)


def far(value):
    return pltpu.with_memory_space_constraint(value, pltpu.HBM)


def swap(value, partner):
    sections, freqs = lax.axis_size("section"), lax.axis_size("freq")
    route = []
    for section in range(sections):
        for freq in range(freqs):
            to_section, to_freq = partner(section, freq)
            route.append((section * freqs + freq, to_section * freqs + to_freq))
    return lax.ppermute(value, BOTH, route)


def search(spectra, channel_gain, bandpass_bin, drift_range, hit_cutoff):
    groups, integrations, chan_dev = spectra.shape
    sections, freqs = lax.axis_size("section"), lax.axis_size("freq")
    section, freq = lax.axis_index("section"), lax.axis_index("freq")
    total_bins = 4 * freqs
    bin_tiles = -(-total_bins // LANES)
    rates = hit_cutoff.shape[1]
    strides = rates // sections
    margin = rates * (integrations - 1)
    cols = chan_dev // LANES
    sizes = Sizes(groups, integrations, bin_tiles, margin, rates, strides)
    blocks = integrations // SUBS
    assert cols % SUBS == 0 and integrations % SUBS == 0 and margin <= LANES - SUBS
    assert sections > 1 and groups * cols == LANES and integrations <= cols
    assert freqs % 2 == 0 and 2 * groups + 1 <= SUBS - 2 and rates % sections == 0
    x = spectra.reshape(groups, blocks, SUBS, cols, LANES).transpose(0, 1, 3, 2, 4)
    x = x.reshape(groups * blocks * cols * SUBS, LANES)
    gain = channel_gain.reshape(cols, LANES)
    bins = bandpass_bin.reshape(cols, LANES)
    shape = functools.partial(jax.ShapeDtypeStruct, dtype=jnp.float32)
    side, _ = pack_count(margin)
    rim_tiles = -(-groups * blocks // side)

    packed, x_near, gain_near, bins_near = pl.pallas_call(
        functools.partial(bin_kernel, groups, integrations, bin_tiles, margin),
        out_shape=(
            shape(((2 * bin_tiles + rim_tiles) * SUBS, LANES)),
            shape(x.shape),
            shape(gain.shape),
            jax.ShapeDtypeStruct(bins.shape, bins.dtype),
        ),
        in_specs=[HBM] * 3,
        out_specs=(VMEM,) * 4,
        scratch_shapes=[pltpu.SemaphoreType.DMA((2 + groups,))],
        compiler_params=PARAMS,
        name="bin_sums",
    )(far(x), far(gain), far(bins))

    turned, cuts = pl.pallas_call(
        functools.partial(turn_kernel, groups, integrations),
        out_shape=(shape((integrations * LANES, LANES)), shape((rates * integrations, LANES))),
        in_specs=[VMEM, HBM, HBM],
        out_specs=(VMEM, VMEM),
        scratch_shapes=[
            pltpu.SMEM(hit_cutoff.shape, jnp.int32),
            pltpu.SMEM(drift_range.shape, jnp.int32),
            pltpu.SemaphoreType.DMA((2,)),
        ],
        compiler_params=PARAMS,
        cost_estimate=pl.CostEstimate(flops=10**7, bytes_accessed=0, transcendentals=0),
        name="turn",
    )(x_near, far(hit_cutoff), far(drift_range))

    mate = lambda s, f: (s, f ^ 1)

    def across(s, f):
        other = f + 1 if f % 2 else f - 1
        if 0 <= other < freqs:
            return (s, other)
        return (s ^ 1, f) if sections % 2 == 0 else (s, f)

    rows = bin_tiles * SUBS
    from_mate = swap(packed, mate)
    pairs = packed[: 2 * rows] + from_mate[: 2 * rows]
    pair, shifted_pair = pairs[:rows], pairs[rows:]
    to_across = jnp.concatenate([pair, packed[2 * rows :]], axis=0)
    to_across, shifted_pair = lax.optimization_barrier((to_across, shifted_pair))
    from_across = swap(to_across, across)
    has_across = jnp.logical_and(freq != 0, freq != freqs - 1)
    own = pair + jnp.where(has_across, from_across[:rows], 0.0)
    if sections == 2:

        def across_other(s, f):
            return (1, across(s, f)[1]) if s == 0 else (0, f ^ 1)

        beside = swap(shifted_pair, lambda s, f: (1 - s, f))
        beside_across = swap(shifted_pair, across_other)
        earlier = beside + jnp.where(has_across, beside_across, 0.0)
        own = own + jnp.where(section == 1, earlier, 0.0)
    else:
        all_shifted = lax.all_gather(shifted_pair, "section")
        is_earlier = lax.broadcasted_iota(jnp.int32, (sections, 1, 1), 0) < section
        earlier = jnp.sum(jnp.where(is_earlier, all_shifted, 0.0), axis=0)
        earlier_across = swap(earlier, across)
        own = own + earlier + jnp.where(has_across, earlier_across, 0.0)
    odd = freq % 2 == 1
    following = jnp.where(odd, own, swap(own, mate))
    next_rim = jnp.where(odd, from_across[rows:], from_mate[2 * rows :])
    next_bins = jnp.where(odd, from_across[SUBS - 2 : SUBS - 1], from_mate[SUBS - 1 : SUBS])

    def work(flops):
        return pl.CostEstimate(flops=flops, bytes_accessed=0, transcendentals=0)

    def later(span):
        half = pltpu.VMEM((integrations // 2 * span, LANES), jnp.float32)
        return [half] * (integrations.bit_length() - 2)

    normal, half_tail, rim_index, head = pl.pallas_call(
        functools.partial(main_kernel, sizes),
        out_shape=(
            shape((integrations * sizes.main_span, LANES)),
            shape((integrations * sizes.tail_span, LANES)),
            jax.ShapeDtypeStruct((sizes.extra, LANES), jnp.int32),
            shape((strides * sizes.head, LANES)),
        ),
        in_specs=[VMEM] * 7,
        out_specs=(VMEM,) * 4,
        scratch_shapes=later(sizes.main_span),
        compiler_params=PARAMS,
        cost_estimate=work(10**7),
        name="main",
    )(gain_near, bins_near, own, next_bins, next_rim, turned, cuts)
    scores_shape = shape((groups * strides * cols, LANES))
    tail, first_scores = pl.pallas_call(
        functools.partial(rim_kernel, sizes),
        out_shape=(shape(half_tail.shape), scores_shape),
        in_specs=[VMEM] * 5,
        out_specs=(VMEM, VMEM),
        scratch_shapes=later(sizes.tail_span),
        compiler_params=PARAMS,
        name="rim",
    )(following, rim_index, half_tail, head, cuts)

    def scores(hop):
        return pl.pallas_call(
            functools.partial(tree_kernel, sizes, hop),
            out_shape=scores_shape,
            in_specs=[VMEM] * 3,
            out_specs=VMEM,
            scratch_shapes=later(sizes.main_span) + later(sizes.tail_span),
            compiler_params=PARAMS,
            cost_estimate=work(10**7),
            name="tree",
        )(normal, tail, cuts)

    arrived = []
    for hop in range(1, sections):
        sent = first_scores if hop == 1 else scores(hop)
        arrived.append(swap(sent, lambda s, f: ((s + hop) % sections, f)))
    parts = [scores(0)] + arrived
    if sections == 2:
        low, high = (jnp.where(section == 0, parts[i], parts[1 - i]) for i in (0, 1))
        out = jnp.concatenate([low, high], axis=0)
    else:
        out = jnp.zeros((sections,) + parts[0].shape, jnp.float32)
        for hop, part in enumerate(parts):
            out = lax.dynamic_update_index_in_dim(out, part, (section + sections - hop) % sections, 0)
    return out.reshape(sections * groups, strides, chan_dev)


def solution(mesh):
    return jax.shard_map(
        search,
        mesh=mesh,
        in_specs=(P("section", None, "freq"), P("freq"), P("freq"), P(), P()),
        out_specs=P(None, "section", "freq"),
        check_vma=False,
    )
```
